128 devices in a mesh: dp: 32 (over x, z_hi, y), expert: 4 (over z_lo, core).
Axes of the slice: x: 4, y: 4, z: 4 (z_hi: 2, z_lo: 2; z = z_hi * 2 + z_lo), core: 2. Of those that a mesh axis runs over, the one named last changes fastest.
Arguments:
- tokens: bfloat16 [16384, 2048], P(('dp', 'expert')), may hold values from -6 to 6
- cotangent: bfloat16 [16384, 2048], P(('dp', 'expert')), may hold values from -6 to 6
- expert_ids: int32 [16384, 2], P(('dp', 'expert')), may hold values from 0 to 3, all different within a row; in each aligned block of 128 rows (0 to 127, 128 to 255, ...) at most 128 rows name the same one
- combine: float32 [16384, 2], P(('dp', 'expert')), may hold values from 0.1 to 1
- w_gate: bfloat16 [4, 2048, 768], P('expert'), may hold values from -0.125 to 0.125
- w_up: bfloat16 [4, 2048, 768], P('expert'), may hold values from -0.125 to 0.125
- w_down: bfloat16 [4, 768, 2048], P('expert'), may hold values from -0.21875 to 0.21875
Outputs:
- input_grad: bfloat16 [16384, 2048], P(('dp', 'expert'))
- combine_grad: float32 [16384, 2], P(('dp', 'expert'))
- gate_grad: bfloat16 [4, 2048, 768], P('expert', 'dp')
- up_grad: bfloat16 [4, 2048, 768], P('expert', 'dp')
- down_grad: bfloat16 [4, 768, 2048], P('expert', 'dp')
The draws below stay inside these ranges and needn't reach their ends.
Inputs may be any that keep to these rules, and one draw needn't show every extreme that they name: `expert_ids`: each token names 2 different experts. In the rows of one device no expert is named by more than 128 tokens, and in some devices' rows some expert is named by exactly 128.
All inputs are finite; a program needn't handle non-finite values.
Results may differ from the reference program's by a relative error of at most 0.02.
Values may be sent and summed in bfloat16 or wider, within the bound.
A program may use at most 128 MiB of HBM per device.

```python
import math
import jax
import jax.numpy as jnp
import numpy as np
from jax import lax

D = 2048
FF = 768
TOK_DEV = 128
TOP = 2
EXPERTS = 4
CAP = 128
TOKENS = 16384
N_DP = 32
N_EXPERT = 4


def steps_of(own_key, shape, split, smallest, largest):
    gain, own = 1.0, jax.random.fold_in(own_key, 6)
    for axis_at, parts in split:
        heights = jnp.exp(jax.random.uniform(jax.random.fold_in(own, axis_at), (parts,), jnp.float32, smallest / len(split), largest / len(split)))
        gain = gain * jnp.repeat(heights, shape[axis_at] // parts).reshape([-1 if axis == axis_at else 1 for axis in range(len(shape))])
    return gain


def deal_out(own_key, own, number, rows, number_of, top, bound, skew):
    ranking = jax.random.permutation(own_key, number_of)
    crowded, common = load_shares(number_of, rows * top, bound, skew, True), load_shares(number_of, rows * top, bound, skew, False)
    places = jnp.arange(number_of)

    def named(lengths, offset_by):
        used = int((lengths > 0).sum())
        fixed = max(1, used // 4)
        shifted = fixed + (places - fixed + offset_by * (used - fixed)) % max(1, number_of - fixed)
        return jnp.zeros((number_of,), jnp.int32).at[ranking[jnp.where(places < fixed, places, shifted)]].set(jnp.asarray(lengths, jnp.int32))

    lengths = jnp.where(number % 4 == 0, named(crowded, number // 4), named(common, number - number // 4 - 1))
    mixed = jax.random.permutation(jax.random.fold_in(own, 3), number_of)
    donor, taker = mixed[0:number_of // 2 * 2:2], mixed[1:number_of // 2 * 2:2]
    room = jnp.minimum(lengths[donor] - 1, bound - lengths[taker]) // 2
    room = jnp.where((donor == ranking[0]) | (taker == ranking[0]) | (lengths[taker] == 0), 0, jnp.maximum(room, 0))
    shifted = jax.random.randint(jax.random.fold_in(own, 4), (number_of // 2,), 0, 1 << 20) % (room + 1)
    lengths = lengths.at[donor].add(-shifted).at[taker].add(shifted)
    items = jnp.searchsorted(jnp.cumsum(lengths), jnp.arange(rows * top), side="right").astype(jnp.int32)
    listing = items.reshape(top, rows).T
    listing = listing[jax.random.permutation(jax.random.fold_in(own, 1), rows)]
    offset_by = jax.random.randint(jax.random.fold_in(own, 2), (rows, 1), 0, top)
    return jnp.take_along_axis(listing, (jnp.arange(top)[None, :] + offset_by) % top, axis=1)


def load_shares(number_of, total, bound, skew, full):
    weights = [(1 << 20) // math.isqrt(standing ** skew) + 1 for standing in range(1, number_of + 1)]
    largest = bound if full else min(bound, max(-(-total // number_of), total * weights[0] // sum(weights)))
    least = 1 if total - largest >= number_of - 1 else 0
    holding, spare = [largest] + [least] * (number_of - 1), total - largest - least * (number_of - 1)
    while spare > 0:
        candidates = [i for i in range(1, number_of) if holding[i] < largest] or [i for i in range(1, number_of) if holding[i] < bound]
        mass, left = sum([weights[i] for i in candidates]), spare
        for i in candidates:
            more = min(bound - holding[i], max(1, left * weights[i] // mass), spare)
            holding[i] = holding[i] + more
            spare = spare - more
    return np.array(holding)


def noise(rng, shape, deviation, reach, split=(), kind=jnp.bfloat16):
    result = jax.random.normal(rng, shape, jnp.float32) * deviation
    if len(split) > 0:
        result = steps_of(rng, shape, split, -0.22, 0.18) * result
    return jnp.clip(result, min=-reach, max=reach).astype(kind)


def setup_inputs(seed: int = 0) -> dict:
    key_list = jax.random.split(jax.random.key(seed), 8)
    tokens = noise(key_list[0], (TOKENS, D), 1.0, 6.0, ((0, 128),))
    cotangent = noise(key_list[1], (TOKENS, D), 1.0, 6.0, ((0, 128),))
    expert_ids_keys = jax.random.split(jax.random.fold_in(key_list[2], 1), TOKENS // TOK_DEV)
    expert_ids_turns = jax.random.permutation(jax.random.fold_in(key_list[2], 3), TOKENS // TOK_DEV)
    expert_ids = jax.vmap(lambda own, number: deal_out(jax.random.fold_in(key_list[2], 2), own, number, TOK_DEV, EXPERTS, TOP, CAP, 2))(expert_ids_keys, expert_ids_turns).reshape((TOKENS, TOP))
    combine = jnp.clip(jnp.exp(math.log(1.0) - 2.3025851 * jax.random.uniform(key_list[3], (TOKENS, TOP), jnp.float32) ** steps_of(key_list[3], (TOKENS, TOP), ((0, 128),), -0.2, 0.2)), 0.1, 1.0)
    w_gate = noise(key_list[4], (EXPERTS, D, FF), D ** -0.5, 0.125, ((0, 4),))
    w_up = noise(key_list[5], (EXPERTS, D, FF), D ** -0.5, 0.125, ((0, 4),))
    w_down = noise(key_list[6], (EXPERTS, FF, D), FF ** -0.5, 0.21875, ((0, 4),))
    return dict(tokens=tokens, cotangent=cotangent, expert_ids=expert_ids, combine=combine, w_gate=w_gate, w_up=w_up, w_down=w_down)


def slot_table(expert_ids, experts_all, capacity):
    pairs = expert_ids.reshape(-1).astype(jnp.int32)
    count = pairs.shape[0]
    onehot = (pairs[:, None] == jnp.arange(experts_all, dtype=jnp.int32)[None, :]).astype(jnp.int32)
    before = jnp.cumsum(onehot, axis=0) - onehot
    position = jnp.sum(before * onehot, axis=1).astype(jnp.int32)
    dest = (pairs * capacity + position).astype(jnp.int32)
    filled = jnp.zeros((experts_all * capacity,), jnp.int32).at[dest].set(jnp.arange(count, dtype=jnp.int32) + 1)
    return dest, filled


def gather_rows(tokens, cotangent, combine, filled, top):
    live = filled > 0
    pair = jnp.maximum(filled - 1, 0).astype(jnp.int32)
    source = (pair // top).astype(jnp.int32)
    rows_x = jnp.where(live[:, None], jnp.take(tokens, source, axis=0), jnp.zeros((), tokens.dtype))
    rows_dy = jnp.where(live[:, None], jnp.take(cotangent, source, axis=0), jnp.zeros((), cotangent.dtype))
    rows_c = jnp.where(live, jnp.take(combine.reshape(-1), pair, axis=0), jnp.zeros((), combine.dtype))
    return rows_x, rows_dy, rows_c


def forward_part(rows_x, gate_mat, up_mat, down_mat):
    gate = jnp.dot(rows_x, gate_mat, preferred_element_type=jnp.float32)
    up = jnp.dot(rows_x, up_mat, preferred_element_type=jnp.float32)
    sig = jax.nn.sigmoid(gate)
    act = gate * sig
    hidden = (act * up).astype(jnp.bfloat16)
    output = jnp.dot(hidden, down_mat, preferred_element_type=jnp.float32)
    return gate, up, sig, act, hidden, output


def backward_part(state, rows_dy, rows_c, gate_mat, up_mat, down_mat):
    gate, up, sig, act, hidden, output = state
    comb_grad = jnp.sum(rows_dy.astype(jnp.float32) * output, axis=1)
    scaled = (rows_c[:, None] * rows_dy.astype(jnp.float32)).astype(jnp.bfloat16)
    last = (((1,), (1,)), ((), ()))
    hidden_grad = lax.dot_general(scaled, down_mat, last, preferred_element_type=jnp.float32)
    gate_d = (hidden_grad * up * (sig * (1.0 + gate * (1.0 - sig)))).astype(jnp.bfloat16)
    up_d = (hidden_grad * act).astype(jnp.bfloat16)
    row_grad = lax.dot_general(gate_d, gate_mat, last, preferred_element_type=jnp.float32)
    row_grad = (row_grad + lax.dot_general(up_d, up_mat, last, preferred_element_type=jnp.float32)).astype(jnp.bfloat16)
    return comb_grad, scaled, gate_d, up_d, row_grad


def reference(tokens, cotangent, expert_ids, combine, w_gate, w_up, w_down):
    first = (((0,), (0,)), ((), ()))
    x_all = tokens.reshape(N_DP, N_EXPERT, TOK_DEV, D)
    dy_all = cotangent.reshape(N_DP, N_EXPERT, TOK_DEV, D)
    id_all = expert_ids.reshape(N_DP, N_EXPERT, TOK_DEV, TOP)
    c_all = combine.reshape(N_DP, N_EXPERT, TOK_DEV, TOP)

    def prepare(x_q, dy_q, id_q, c_q):
        dest, filled = slot_table(id_q, EXPERTS, CAP)
        rows_x, rows_dy, rows_c = gather_rows(x_q, dy_q, c_q, filled, TOP)
        return dest, rows_x.reshape(EXPERTS, CAP, D), rows_dy.reshape(EXPERTS, CAP, D), rows_c.reshape(EXPERTS, CAP)

    def one_expert(item):
        inputs, cot_rows, comb_rows, gate_mat, up_mat, down_mat = item
        state = forward_part(inputs, gate_mat, up_mat, down_mat)
        comb_grad, scaled, gate_d, up_d, row_grad = backward_part(state, cot_rows, comb_rows, gate_mat, up_mat, down_mat)
        gate_part = lax.dot_general(inputs, gate_d, first, preferred_element_type=jnp.float32).astype(jnp.bfloat16)
        up_part = lax.dot_general(inputs, up_d, first, preferred_element_type=jnp.float32).astype(jnp.bfloat16)
        down_part = lax.dot_general(state[4], scaled, first, preferred_element_type=jnp.float32).astype(jnp.bfloat16)
        return row_grad, comb_grad, gate_part, up_part, down_part

    def finish(flat_rows, flat_comb, dest):
        picked = jnp.take(flat_rows, dest, axis=0).reshape(TOK_DEV, TOP, D)
        summed = jnp.sum(picked.astype(jnp.float32), axis=1).astype(jnp.bfloat16)
        return summed, jnp.take(flat_comb, dest, axis=0).reshape(TOK_DEV, TOP)

    def one_replica(carry, inputs):
        x_r, dy_r, id_r, c_r = inputs
        dest, rx, rdy, rc = jax.vmap(prepare)(x_r, dy_r, id_r, c_r)
        group_x = jnp.transpose(rx, (1, 0, 2, 3)).reshape(EXPERTS, N_EXPERT * CAP, D)
        group_dy = jnp.transpose(rdy, (1, 0, 2, 3)).reshape(EXPERTS, N_EXPERT * CAP, D)
        group_c = jnp.transpose(rc, (1, 0, 2)).reshape(EXPERTS, N_EXPERT * CAP)
        rows, combs, gate_part, up_part, down_part = lax.map(one_expert, (group_x, group_dy, group_c, w_gate, w_up, w_down))
        gate_part, up_part, down_part = lax.optimization_barrier((gate_part, up_part, down_part))
        carry = (carry[0] + gate_part.astype(jnp.float32), carry[1] + up_part.astype(jnp.float32), carry[2] + down_part.astype(jnp.float32))
        back = jnp.transpose(rows.reshape(EXPERTS, N_EXPERT, CAP, D), (1, 0, 2, 3)).reshape(N_EXPERT, EXPERTS * CAP, D)
        back_c = jnp.transpose(combs.reshape(EXPERTS, N_EXPERT, CAP), (1, 0, 2)).reshape(N_EXPERT, EXPERTS * CAP)
        grads_in, grads_c = jax.vmap(finish)(back, back_c, dest)
        return carry, (grads_in, grads_c)

    start = (jnp.zeros((EXPERTS, D, FF), jnp.float32), jnp.zeros((EXPERTS, D, FF), jnp.float32), jnp.zeros((EXPERTS, FF, D), jnp.float32))
    sums, (grads_in, grads_c) = lax.scan(one_replica, start, (x_all, dy_all, id_all, c_all))
    input_grad = grads_in.reshape(TOKENS, D)
    combine_grad = grads_c.reshape(TOKENS, TOP)
    return (input_grad, combine_grad, sums[0].astype(jnp.bfloat16), sums[1].astype(jnp.bfloat16), sums[2].astype(jnp.bfloat16))
```

```python
import jax
import jax.numpy as jnp
from jax import lax
from jax.experimental import pallas as pl
from jax.experimental.pallas import tpu as pltpu
from jax.sharding import PartitionSpec as P

MESH = pl.DeviceIdType.MESH
BF16 = jnp.bfloat16
F32 = jnp.float32
D = 2048
FF = 768
T = 128
N_SEM = 160


def mod4(v):
    return lax.rem(v + 8, 4)


def nt(a, b):
    return lax.dot_general(a, b, (((1,), (1,)), ((), ())), preferred_element_type=F32)


def nn(a, b):
    return jnp.dot(a, b, preferred_element_type=F32)


class Wire:
    def __init__(self, send, recv):
        self.send, self.recv, self.count, self.all = send, recv, 0, []

    def make(self, src, dst, device):
        i = self.count
        self.count += 1
        copy = pltpu.make_async_remote_copy(
            src_ref=src,
            dst_ref=dst,
            send_sem=self.send.at[i],
            recv_sem=self.recv.at[i],
            device_id=device,
            device_id_type=MESH,
        )
        self.all.append(copy)
        copy.start()
        return copy


class Stream:
    def __init__(self, first, partial, recv1, gathered, recv2, recv3):
        self.first, self.partial, self.recv1 = first, partial, recv1
        self.gathered, self.recv2, self.recv3 = gathered, recv2, recv3
        self.flight = {}

    def chunk(self, way, c):
        return (c, way) if self.first == "x" else (slice(None), way, c)


def kernel(
    x_hbm,
    dy_hbm,
    ids_ref,
    comb_ref,
    wg_hbm,
    wu_hbm,
    wd_hbm,
    ig_ref,
    cg_ref,
    gg_ref,
    ug_ref,
    dg_ref,
    wg,
    wu,
    wd,
    x,
    dy,
    xt,
    act,
    dact,
    hid,
    hg,
    hc,
    hct,
    gd,
    ud,
    weight_rows,
    weight_cols,
    cg_part,
    cg_rows,
    cg_in,
    rg,
    rc,
    rz,
    pd,
    pg,
    rd1,
    rg1,
    qd,
    rd2,
    rg2,
    rd3,
    rg3,
    local_sem,
    send_sem,
    recv_sem,
):
    dp, ex = lax.axis_index("dp"), lax.axis_index("expert")
    ix, zh, iy = lax.div(dp, 8), lax.rem(lax.div(dp, 4), 2), lax.rem(dp, 4)
    zl, core = lax.div(ex, 2), lax.rem(ex, 2)

    def at(a, b, c):
        return {"dp": a * 8 + b * 4 + c, "expert": ex}

    x_next, x_prev = at(mod4(ix + 1), zh, iy), at(mod4(ix - 1), zh, iy)
    y_next, y_prev = at(ix, zh, mod4(iy + 1)), at(ix, zh, mod4(iy - 1))
    z_far = at(ix, 1 - zh, iy)
    mate = {"dp": dp, "expert": zl * 2 + 1 - core}
    z_near = {"dp": dp, "expert": (1 - zl) * 2 + core}
    z_diag = {"dp": dp, "expert": (1 - zl) * 2 + 1 - core}

    loads = [
        pltpu.make_async_copy(x_hbm, x.at[pl.ds(0, T)], local_sem.at[0]),
        pltpu.make_async_copy(dy_hbm, dy.at[pl.ds(0, T)], local_sem.at[1]),
        pltpu.make_async_copy(wg_hbm.at[0], wg, local_sem.at[2]),
        pltpu.make_async_copy(wu_hbm.at[0], wu, local_sem.at[3]),
        pltpu.make_async_copy(wd_hbm.at[0], wd, local_sem.at[4]),
    ]
    for load in loads:
        load.start()

    barrier = pltpu.get_barrier_semaphore()
    peers = (x_next, x_prev, y_next, y_prev, z_far, mate, z_near, z_diag)
    for peer in peers:
        pl.semaphore_signal(barrier, inc=1, device_id=peer, device_id_type=MESH)
    pl.semaphore_wait(barrier, len(peers))

    wire = Wire(send_sem, recv_sem)

    loads[0].wait()
    x_mate = wire.make(x.at[pl.ds(0, T)], x.at[pl.ds(T, T)], mate)
    x_near = [
        wire.make(x.at[pl.ds(64 * j, 64)], x.at[pl.ds(2 * T + 64 * j, 64)], z_near)
        for j in range(2)
    ]
    loads[1].wait()
    dy_mate = wire.make(dy.at[pl.ds(0, T)], dy.at[pl.ds(T, T)], mate)
    lane = lax.broadcasted_iota(jnp.int32, (T, T), 1)
    dense = jnp.zeros((T, T), F32)
    for k in range(2):
        dense += jnp.where(ids_ref[:, k : k + 1] == lane, comb_ref[:, k : k + 1], 0.0)
    weight_rows[0] = jnp.transpose(dense)[0:8]
    w_in = [
        wire.make(weight_rows.at[0], weight_rows.at[j], to)
        for j, to in ((1, mate), (2, z_near), (3, z_diag))
    ]
    dy_near = [
        wire.make(dy.at[pl.ds(32 * j, 32)], dy.at[pl.ds(2 * T + 32 * j, 32)], z_near)
        for j in range(4)
    ]

    def pass_on(arrivals, ref, rows):
        out = []
        for j, arrival in enumerate(arrivals):
            arrival.wait_recv()
            out.append(
                wire.make(
                    ref.at[pl.ds(2 * T + rows * j, rows)],
                    ref.at[pl.ds(3 * T + rows * j, rows)],
                    mate,
                )
            )
        return out

    def column_weights(slot):
        row = weight_rows[slot, pl.ds(ex, 1), :]
        weight_cols[slot * T : slot * T + T, :] = jnp.transpose(jnp.broadcast_to(row, (T, T)))

    def spread(start):
        col = weight_cols[pl.ds(start, 16), :]
        return jnp.concatenate([col] * 6, axis=1)

    def turned(r0):
        def body(j, carry):
            cols = pl.ds(pl.multiple_of(j * 256, 256), 256)
            xt[cols, r0 : r0 + 256] = jnp.transpose(x[r0 : r0 + 256, cols])
            return carry

        lax.fori_loop(0, D // 256, body, 0)

    def forward(r0):
        def matmul(n, carry):
            cols = pl.ds(pl.multiple_of(n * 256, 256), 256)
            act[:, cols] = nn(x[r0 : r0 + 256, :], wg[:, cols])
            dact[:, cols] = nn(x[r0 : r0 + 256, :], wu[:, cols])
            return carry

        lax.fori_loop(0, FF // 256, matmul, 0)

        def pointwise(i, carry):
            rows = pl.ds(pl.multiple_of(i * 16, 16), 16)
            gate, up = act[rows, :], dact[rows, :]
            s = jax.nn.sigmoid(gate)
            a = gate * s
            h = a * up
            act[rows, :] = a
            dact[rows, :] = up * s * (1.0 + gate * (1.0 - s))
            hid[rows, :] = h
            hc[rows, :] = (h * spread(pl.multiple_of(r0 + i * 16, 16))).astype(BF16)
            return carry

        lax.fori_loop(0, 16, pointwise, 0)

        def turn(n, carry):
            cols = pl.ds(pl.multiple_of(n * 256, 256), 256)
            hct[cols, r0 : r0 + 256] = jnp.transpose(hc[:, cols])
            return carry

        lax.fori_loop(0, FF // 256, turn, 0)

    def backward(r0):
        def matmul(n, carry):
            cols = pl.ds(pl.multiple_of(n * 256, 256), 256)
            hg[:, cols] = nt(dy[r0 : r0 + 256, :], wd[cols, :])
            return carry

        lax.fori_loop(0, FF // 256, matmul, 0)

        def pointwise(i, carry):
            rows = pl.ds(pl.multiple_of(i * 16, 16), 16)
            full = pl.ds(pl.multiple_of(r0 + i * 16, 16), 16)
            g = hg[rows, :]
            prod = g * hid[rows, :]
            total = prod[:, 0:128]
            for j in range(1, 6):
                total += prod[:, 128 * j : 128 * j + 128]
            cg_part[full, :] = total
            g = g * spread(pl.multiple_of(r0 + i * 16, 16))
            gd[full, :] = (g * dact[rows, :]).astype(BF16)
            ud[full, :] = (g * act[rows, :]).astype(BF16)
            return carry

        lax.fori_loop(0, 16, pointwise, 0)

    loads[2].wait()
    loads[3].wait()
    x_mate.wait_recv()
    for copy in w_in:
        copy.wait_recv()
    for slot in range(4):
        column_weights(slot)
    forward(0)
    x_diag = pass_on(x_near[0:1], x, 64)
    turned(0)
    loads[4].wait()
    dy_mate.wait_recv()
    backward(0)
    x_near[1].wait_recv()
    x_diag.append(
        wire.make(x.at[pl.ds(2 * T + 64, 64)], x.at[pl.ds(3 * T + 64, 64)], mate)
    )

    for copy in x_diag:
        copy.wait_recv()
    forward(256)
    turned(256)
    dy_diag = pass_on(dy_near, dy, 32)
    for copy in dy_diag:
        copy.wait_recv()

    def stream(first, partial, recv1, gathered, recv2, recv3):
        return Stream(first, partial, recv1, gathered, recv2, recv3)

    d0 = stream("x", pd.at[0], rd1.at[0], qd.at[0], rd2.at[0], rd3.at[0])
    d1 = stream("x", pd.at[1], rd1.at[1], qd.at[1], rd2.at[1], rd3.at[1])
    g0 = stream("x", pg.at[0], rg1.at[0], None, rg2.at[0], rg3.at[0])
    g1 = stream("y", pg.at[1], rg1.at[1], None, rg2.at[1], rg3.at[1])
    u0 = stream("y", pg.at[2], rg1.at[2], None, rg2.at[2], rg3.at[2])
    u1 = stream("y", pg.at[3], rg1.at[3], None, rg2.at[3], rg3.at[3])

    def down_part(dst, c0):
        def body(n, carry):
            src = pl.ds(pl.multiple_of(c0 + n * 256, 256), 256)
            cols = pl.ds(pl.multiple_of(n * 256, 256), 256)
            r = nn(hct[...], dy[:, src]).astype(BF16)
            dst[:, :, :, cols] = r.reshape(4, 2, 96, 256)
            return carry

        lax.fori_loop(0, 4, body, 0)

    def up_part(dst, right, c0):
        def body(m, carry):
            rows = pl.ds(pl.multiple_of(m * 256, 256), 256)
            r = nn(xt[rows, :], right[:, c0 : c0 + 384]).astype(BF16)
            dst[lax.div(m, 2), lax.rem(m, 2)] = r.reshape(4, 64, 384)
            return carry

        lax.fori_loop(0, 8, body, 0)

    def ring1(st, way):
        i = ix if st.first == "x" else iy
        sign = 1 - 2 * way
        near = ((x_next, x_prev) if st.first == "x" else (y_next, y_prev))[way]
        return i, sign, near

    def ring2(st, way):
        i = iy if st.first == "x" else ix
        sign = 1 - 2 * way
        near = ((y_next, y_prev) if st.first == "x" else (x_next, x_prev))[way]
        return i, sign, near

    def launch(st):
        for way in range(2):
            i, sign, near = ring1(st, way)
            c = mod4(i - sign)
            src = st.partial.at[st.chunk(way, c)]
            st.flight[way] = wire.make(src, st.recv1.at[way, 0], near)

    def settled(st, way, c):
        return st.gathered.at[way, c] if st.gathered is not None else st.recv1.at[way, 2, c]

    def step1(st, s):
        for way in range(2):
            i, sign, near = ring1(st, way)
            c = mod4(i - (2 + s) * sign)
            st.flight[way].wait_recv()
            if st.gathered is None:
                for j in range(4):
                    own = st.partial[c, way, j] if st.first == "x" else st.partial[j, way, c]
                    total = st.recv1[way, s, j].astype(F32) + own.astype(F32)
                    st.recv1[way, s, j] = total.astype(BF16)
            elif s < 2:
                for j in range(4):
                    cols = slice(256 * j, 256 * j + 256)
                    total = st.recv1[way, s, :, cols].astype(F32)
                    total += st.partial[c, way, :, cols].astype(F32)
                    st.recv1[way, s, :, cols] = total.astype(BF16)
            else:
                for j in range(2):
                    lo = slice(256 * j, 256 * j + 256)
                    hi = slice(512 + 256 * j, 768 + 256 * j)
                    left = st.recv1[way, s, :, lo].astype(F32)
                    left += st.partial[c, way, :, lo].astype(F32)
                    right = st.recv1[way, s, :, hi].astype(F32)
                    right += st.partial[c, way, :, hi].astype(F32)
                    for q in range(4):
                        both = jnp.concatenate(
                            [left[24 * q : 24 * q + 24], right[24 * q : 24 * q + 24]], axis=0
                        )
                        st.gathered[way, q, :, lo] = both.astype(BF16)
            if s < 2:
                st.flight[way] = wire.make(st.recv1.at[way, s], st.recv1.at[way, s + 1], near)
            else:
                i, sign, near = ring2(st, way)
                src = settled(st, way, mod4(i - sign))
                st.flight[way] = wire.make(src, st.recv2.at[way, 0], near)

    def step2(st, s):
        for way in range(2):
            i, sign, near = ring2(st, way)
            c = mod4(i - (2 + s) * sign)
            st.flight[way].wait_recv()
            total = st.recv2[way, s].astype(F32) + settled(st, way, c)[...].astype(F32)
            st.recv2[way, s] = total.astype(BF16)
            if s < 2:
                st.flight[way] = wire.make(st.recv2.at[way, s], st.recv2.at[way, s + 1], near)
        if s == 2:
            st.flight[2] = wire.make(st.recv2.at[1 - zh, 2], st.recv3, z_far)

    def result(st):
        st.flight[2].wait_recv()
        return st.recv2[zh, 2].astype(F32) + st.recv3[...].astype(F32)

    down_part(d0.partial, 0)
    launch(d0)
    backward(256)
    up_part(g1.partial, gd, 384)
    launch(g1)
    down_part(d1.partial, 1024)
    launch(d1)
    up_part(u0.partial, ud, 0)
    launch(u0)
    up_part(g0.partial, gd, 0)
    launch(g0)
    up_part(u1.partial, ud, 384)
    launch(u1)

    def row_part(r0):
        def body(n, carry):
            cols = pl.ds(pl.multiple_of(n * 256, 256), 256)
            r = nt(gd[r0 : r0 + 256, :], wg[cols, :]) + nt(ud[r0 : r0 + 256, :], wu[cols, :])
            rg[r0 : r0 + 256, cols] = r.astype(BF16)
            return carry

        lax.fori_loop(0, D // 256, body, 0)

    order = (d0, g1, d1, u0, g0, u1)
    for st in order[0:2]:
        step1(st, 0)
    row_part(256)
    rc_far = wire.make(rg.at[pl.ds(3 * T, T)], rc.at[1], mate)
    for slot in range(4):
        row = jnp.sum(jnp.transpose(cg_part[slot * T : slot * T + T, :]), axis=0, keepdims=True)
        cg_rows[slot] = jnp.broadcast_to(row, (8, T))
    cg_copies = [
        wire.make(cg_rows.at[j], cg_in.at[j], to)
        for j, to in ((1, mate), (2, z_near), (3, z_diag))
    ]
    for st in order[2:4]:
        step1(st, 0)
    row_part(0)
    rc_near = wire.make(rg.at[pl.ds(T, T)], rc.at[0], mate)
    for st in order[4:6]:
        step1(st, 0)
    rc_far.wait_recv()

    def add_far(i, carry):
        rows = pl.ds(pl.multiple_of(i * 16, 16), 16)
        full = pl.ds(pl.multiple_of(2 * T + i * 16, 16), 16)
        total = rg[full, :].astype(F32) + rc[1, rows, :].astype(F32)
        rg[full, :] = total.astype(BF16)
        return carry

    lax.fori_loop(0, T // 16, add_far, 0)
    rz_in = wire.make(rg.at[pl.ds(2 * T, T)], rz, z_near)

    for st in order:
        step1(st, 1)

    ids = ids_ref[...]
    for copy in cg_copies:
        copy.wait_recv()
    answer = jnp.zeros((T, 2), F32)
    for j in range(4):
        row = cg_rows[0, 0:1, :] if j == 0 else cg_in[j, 0:1, :]
        cols = jnp.transpose(jnp.broadcast_to(row, (T, T)))[:, 0:2]
        answer += jnp.where(ids == jnp.bitwise_xor(ex, j), cols, 0.0)
    cg_ref[...] = answer

    for st in order:
        step1(st, 2)

    rc_near.wait_recv()
    rz_in.wait_recv()

    def add_rows(i, carry):
        rows = pl.ds(pl.multiple_of(i * 16, 16), 16)
        total = rg[rows, :].astype(F32) + rc[0, rows, :].astype(F32) + rz[rows, :].astype(F32)
        ig_ref[rows, :] = total.astype(BF16)
        return carry

    lax.fori_loop(0, T // 16, add_rows, 0)

    for s in range(3):
        for st in order:
            step2(st, s)
    for st, base in ((d0, 0), (d1, 1024)):
        r = result(st)
        dg_ref[0, :, base : base + 512] = r[0:24].astype(BF16)
        dg_ref[0, :, base + 512 : base + 1024] = r[24:48].astype(BF16)
    gg_ref[0, :, 384:768] = result(g1).astype(BF16)
    ug_ref[0, :, 0:384] = result(u0).astype(BF16)
    gg_ref[0, :, 0:384] = result(g0).astype(BF16)
    ug_ref[0, :, 384:768] = result(u1).astype(BF16)

    for copy in wire.all:
        copy.wait_send()


def shards(tokens, cotangent, expert_ids, combine, w_gate, w_up, w_down):
    hbm = pl.BlockSpec(memory_space=pl.ANY)
    vmem = pl.BlockSpec(memory_space=pltpu.VMEM)
    return pl.pallas_call(
        kernel,
        out_shape=(
            jax.ShapeDtypeStruct((T, D), BF16),
            jax.ShapeDtypeStruct((T, 2), F32),
            jax.ShapeDtypeStruct((1, 64, FF), BF16),
            jax.ShapeDtypeStruct((1, 64, FF), BF16),
            jax.ShapeDtypeStruct((1, 24, D), BF16),
        ),
        in_specs=[hbm, hbm, vmem, vmem, hbm, hbm, hbm],
        out_specs=(vmem, vmem, vmem, vmem, vmem),
        scratch_shapes=[
            pltpu.VMEM((D, FF), BF16),
            pltpu.VMEM((D, FF), BF16),
            pltpu.VMEM((FF, D), BF16),
            pltpu.VMEM((4 * T, D), BF16),
            pltpu.VMEM((4 * T, D), BF16),
            pltpu.VMEM((D, 4 * T), BF16),
            pltpu.VMEM((256, FF), F32),
            pltpu.VMEM((256, FF), F32),
            pltpu.VMEM((256, FF), F32),
            pltpu.VMEM((256, FF), F32),
            pltpu.VMEM((256, FF), BF16),
            pltpu.VMEM((FF, 4 * T), BF16),
            pltpu.VMEM((4 * T, FF), BF16),
            pltpu.VMEM((4 * T, FF), BF16),
            pltpu.VMEM((4, 8, T), F32),
            pltpu.VMEM((4 * T, T), F32),
            pltpu.VMEM((4 * T, T), F32),
            pltpu.VMEM((4, 8, T), F32),
            pltpu.VMEM((4, 8, T), F32),
            pltpu.VMEM((4 * T, D), BF16),
            pltpu.VMEM((2, T, D), BF16),
            pltpu.VMEM((T, D), BF16),
            pltpu.VMEM((2, 4, 2, 96, 1024), BF16),
            pltpu.VMEM((4, 4, 2, 4, 64, 384), BF16),
            pltpu.VMEM((2, 2, 3, 96, 1024), BF16),
            pltpu.VMEM((4, 2, 3, 4, 64, 384), BF16),
            pltpu.VMEM((2, 2, 4, 48, 512), BF16),
            pltpu.VMEM((2, 2, 3, 48, 512), BF16),
            pltpu.VMEM((4, 2, 3, 64, 384), BF16),
            pltpu.VMEM((2, 48, 512), BF16),
            pltpu.VMEM((4, 64, 384), BF16),
            pltpu.SemaphoreType.DMA((5,)),
            pltpu.SemaphoreType.DMA((N_SEM,)),
            pltpu.SemaphoreType.DMA((N_SEM,)),
        ],
        compiler_params=pltpu.CompilerParams(
            collective_id=0, has_side_effects=True, vmem_limit_bytes=62 * 1024 * 1024
        ),
        name="experts",
    )(tokens, cotangent, expert_ids, combine, w_gate, w_up, w_down)


def solution(mesh):
    both = ("dp", "expert")
    return jax.shard_map(
        shards,
        mesh=mesh,
        in_specs=(
            P(both, None),
            P(both, None),
            P(both, None),
            P(both, None),
            P("expert", None, None),
            P("expert", None, None),
            P("expert", None, None),
        ),
        out_specs=(
            P(both, None),
            P(both, None),
            P("expert", "dp", None),
            P("expert", "dp", None),
            P("expert", "dp", None),
        ),
        check_vma=False,
    )
```

```python
import jax
import jax.numpy as jnp
from jax import lax
from jax.experimental import pallas as pl
from jax.experimental.pallas import tpu as pltpu
from jax.sharding import PartitionSpec as P

MESH = pl.DeviceIdType.MESH
BF16 = jnp.bfloat16
F32 = jnp.float32
D = 2048
FF = 768
T = 128
N_SEM = 140


def mod4(v):
    return lax.rem(v + 8, 4)


def nt(a, b):
    return lax.dot_general(a, b, (((1,), (1,)), ((), ())), preferred_element_type=F32)


def nn(a, b):
    return jnp.dot(a, b, preferred_element_type=F32)


class Wire:
    def __init__(self, sems, other):
        self.sems, self.other, self.count, self.groups = sems, other, 0, []

    def sem(self):
        self.count += 1
        return self.sems.at[self.count - 1]

    def describe(self, src, dst, send, recv, device):
        return pltpu.make_async_remote_copy(
            src_ref=src,
            dst_ref=dst,
            send_sem=send,
            recv_sem=recv,
            device_id=device,
            device_id_type=MESH,
        )

    def group(self, total):
        send = self.sem()
        self.groups.append((send, total))
        return send

    def put(self, src, dst, device, send, recv):
        self.describe(src, dst, send, recv, device).start()

    def arrived(self, ref, recv):
        self.describe(ref, ref, recv, recv, self.other).wait_recv()

    def finish(self):
        for send, total in self.groups:
            self.describe(total, total, send, send, self.other).wait_send()


class Stream:
    def __init__(self, wire, first, partial, recv1, recv2, recv3):
        self.first, self.partial = first, partial
        self.recv1, self.recv2, self.recv3 = recv1, recv2, recv3
        self.send1, self.send2 = wire.group(recv1), wire.group(recv2)
        self.send3 = wire.group(recv3)
        self.sem1 = [wire.sem() for _ in range(3)]
        self.sem2 = [wire.sem() for _ in range(3)]
        self.sem3 = wire.sem()

    def chunk(self, way, c):
        return (c, way) if self.first == "x" else (slice(None), way, c)


def kernel(
    x_hbm,
    dy_hbm,
    ids_ref,
    comb_ref,
    wg_hbm,
    wu_hbm,
    wd_hbm,
    ig_hbm,
    cg_hbm,
    gg_hbm,
    ug_hbm,
    dg_hbm,
    wg,
    wu,
    wd,
    x,
    dy,
    xt,
    act,
    dact,
    hid,
    hg,
    hc,
    hct,
    gd,
    ud,
    weight_rows,
    weight_cols,
    cg_part,
    cg_rows,
    cg_in,
    rg,
    rc,
    rz,
    pd,
    pg,
    rd1,
    rg1,
    rd2,
    rg2,
    rd3,
    rg3,
    ig_out,
    cg_out,
    gg_out,
    ug_out,
    dg_out,
    local_sem,
    remote_sem,
):
    dp, ex = lax.axis_index("dp"), lax.axis_index("expert")
    ix, zh, iy = lax.div(dp, 8), lax.rem(lax.div(dp, 4), 2), lax.rem(dp, 4)
    zl, core = lax.div(ex, 2), lax.rem(ex, 2)

    def at(a, b, c):
        return {"dp": a * 8 + b * 4 + c, "expert": ex}

    x_next, x_prev = at(mod4(ix + 1), zh, iy), at(mod4(ix - 1), zh, iy)
    y_next, y_prev = at(ix, zh, mod4(iy + 1)), at(ix, zh, mod4(iy - 1))
    z_far = at(ix, 1 - zh, iy)
    mate = {"dp": dp, "expert": zl * 2 + 1 - core}
    z_near = {"dp": dp, "expert": (1 - zl) * 2 + core}
    z_diag = {"dp": dp, "expert": (1 - zl) * 2 + 1 - core}

    loads = [
        pltpu.make_async_copy(x_hbm, x.at[pl.ds(0, T)], local_sem.at[0]),
        pltpu.make_async_copy(dy_hbm, dy.at[pl.ds(0, T)], local_sem.at[1]),
        pltpu.make_async_copy(wg_hbm.at[0], wg, local_sem.at[2]),
        pltpu.make_async_copy(wu_hbm.at[0], wu, local_sem.at[3]),
        pltpu.make_async_copy(wd_hbm.at[0], wd, local_sem.at[4]),
    ]
    for load in loads:
        load.start()

    barrier = pltpu.get_barrier_semaphore()
    peers = (x_next, x_prev, y_next, y_prev, z_far, mate, z_near, z_diag)
    for peer in peers:
        pl.semaphore_signal(barrier, inc=1, device_id=peer, device_id_type=MESH)
    pl.semaphore_wait(barrier, len(peers))

    wire = Wire(remote_sem, mate)

    def slot_rows(ref, slot):
        return ref.at[pl.ds(slot * T, T)]

    def x_block(slot, j):
        return x.at[pl.ds(slot * T + 64 * j, 64)]

    def dy_block(slot, j):
        return dy.at[pl.ds(slot * T, T), pl.ds(512 * j, 512)]

    x_near_send, x_near = wire.group(slot_rows(x, 0)), [wire.sem() for _ in range(2)]
    x_mate_send, x_mate = wire.group(slot_rows(x, 0)), wire.sem()
    x_pass_send, x_diag = wire.group(slot_rows(x, 2)), [wire.sem() for _ in range(2)]
    dy_near_send, dy_near = wire.group(slot_rows(dy, 0)), [wire.sem() for _ in range(4)]
    dy_mate_send, dy_mate = wire.group(slot_rows(dy, 0)), wire.sem()
    dy_pass_send, dy_diag = wire.group(slot_rows(dy, 2)), [wire.sem() for _ in range(4)]
    w_send, w_in = wire.group(weight_rows.at[pl.ds(1, 3)]), wire.sem()

    expert = lax.broadcasted_iota(jnp.int32, (8, T), 0)
    dense = jnp.zeros((8, T), F32)
    for k in range(2):
        dense += jnp.where(ids_ref[k : k + 1, :] == expert, comb_ref[k : k + 1, :], 0.0)
    weight_rows[0] = dense
    for j, to in ((1, mate), (2, z_near), (3, z_diag)):
        wire.put(weight_rows.at[0], weight_rows.at[j], to, w_send, w_in)

    loads[0].wait()
    for j in range(2):
        wire.put(x_block(0, j), x_block(2, j), z_near, x_near_send, x_near[j])
    wire.put(slot_rows(x, 0), slot_rows(x, 1), mate, x_mate_send, x_mate)
    loads[1].wait()
    for j in range(4):
        wire.put(dy_block(0, j), dy_block(2, j), z_near, dy_near_send, dy_near[j])
    wire.put(slot_rows(dy, 0), slot_rows(dy, 1), mate, dy_mate_send, dy_mate)

    def pass_x(j):
        wire.arrived(x_block(2, j), x_near[j])
        wire.put(x_block(2, j), x_block(3, j), mate, x_pass_send, x_diag[j])

    def pass_dy(j):
        wire.arrived(dy_block(2, j), dy_near[j])
        wire.put(dy_block(2, j), dy_block(3, j), mate, dy_pass_send, dy_diag[j])

    def column_weights(slot):
        row = weight_rows[slot, pl.ds(ex, 1), :]
        weight_cols[slot * T : slot * T + T, :] = jnp.transpose(jnp.broadcast_to(row, (T, T)))

    def spread(start):
        col = weight_cols[pl.ds(start, 16), :]
        return jnp.concatenate([col] * 6, axis=1)

    def turned(r0):
        def body(j, carry):
            cols = pl.ds(pl.multiple_of(j * 256, 256), 256)
            xt[cols, r0 : r0 + 256] = jnp.transpose(x[r0 : r0 + 256, cols])
            return carry

        lax.fori_loop(0, D // 256, body, 0)

    def forward(r0):
        def matmul(n, carry):
            cols = pl.ds(pl.multiple_of(n * 256, 256), 256)
            act[:, cols] = nn(x[r0 : r0 + 256, :], wg[:, cols])
            dact[:, cols] = nn(x[r0 : r0 + 256, :], wu[:, cols])
            return carry

        lax.fori_loop(0, FF // 256, matmul, 0)

        def pointwise(i, carry):
            rows = pl.ds(pl.multiple_of(i * 16, 16), 16)
            gate, up = act[rows, :], dact[rows, :]
            s = jax.nn.sigmoid(gate)
            a = gate * s
            h = a * up
            act[rows, :] = a
            dact[rows, :] = up * s * (1.0 + gate * (1.0 - s))
            hid[rows, :] = h
            hc[rows, :] = (h * spread(pl.multiple_of(r0 + i * 16, 16))).astype(BF16)
            return carry

        lax.fori_loop(0, 16, pointwise, 0)

        def turn(n, carry):
            cols = pl.ds(pl.multiple_of(n * 256, 256), 256)
            hct[cols, r0 : r0 + 256] = jnp.transpose(hc[:, cols])
            return carry

        lax.fori_loop(0, FF // 256, turn, 0)

    def hidden_part(r0, first, j0, width):
        def matmul(n, carry):
            cols = pl.ds(pl.multiple_of(n * 256, 256), 256)
            r = nt(dy[r0 : r0 + 256, j0 : j0 + width], wd[cols, j0 : j0 + width])
            hg[:, cols] = r if first else hg[:, cols] + r
            return carry

        lax.fori_loop(0, FF // 256, matmul, 0)

    def backward(r0):
        def pointwise(i, carry):
            rows = pl.ds(pl.multiple_of(i * 16, 16), 16)
            full = pl.ds(pl.multiple_of(r0 + i * 16, 16), 16)
            g = hg[rows, :]
            prod = g * hid[rows, :]
            total = prod[:, 0:128]
            for j in range(1, 6):
                total += prod[:, 128 * j : 128 * j + 128]
            cg_part[full, :] = total
            g = g * spread(pl.multiple_of(r0 + i * 16, 16))
            gd[full, :] = (g * dact[rows, :]).astype(BF16)
            ud[full, :] = (g * act[rows, :]).astype(BF16)
            return carry

        lax.fori_loop(0, 16, pointwise, 0)

    loads[2].wait()
    loads[3].wait()
    wire.arrived(slot_rows(x, 1), x_mate)
    wire.arrived(weight_rows.at[pl.ds(1, 3)], w_in)
    for slot in range(4):
        column_weights(slot)
    forward(0)
    pass_x(0)
    turned(0)
    loads[4].wait()
    wire.arrived(slot_rows(dy, 1), dy_mate)
    hidden_part(0, True, 0, D)
    backward(0)
    pass_x(1)

    for j in range(2):
        wire.arrived(x_block(3, j), x_diag[j])
    forward(256)

    def down_stream(first, j):
        return Stream(wire, first, pd.at[j], rd1.at[j], rd2.at[j], rd3.at[j])

    def up_stream(first, j):
        return Stream(wire, first, pg.at[j], rg1.at[j], rg2.at[j], rg3.at[j])

    d = [down_stream(first, j) for j, first in enumerate("xyxy")]
    g0, g1, u0, u1 = [up_stream(first, j) for j, first in enumerate("xyxy")]

    def down_part(dst, c0):
        def body(n, carry):
            src = pl.ds(pl.multiple_of(c0 + n * 256, 256), 256)
            cols = pl.ds(pl.multiple_of(n * 256, 256), 256)
            r = nn(hct[...], dy[:, src]).reshape(4, 2, 4, 24, 256)
            dst[:, :, :, :, cols] = r.astype(BF16)
            return carry

        lax.fori_loop(0, 2, body, 0)

    def up_part(dst, right, c0):
        def body(m, carry):
            rows = pl.ds(pl.multiple_of(m * 256, 256), 256)
            r = nn(xt[rows, :], right[:, c0 : c0 + 384]).astype(BF16)
            dst[lax.div(m, 2), lax.rem(m, 2)] = r.reshape(4, 64, 384)
            return carry

        lax.fori_loop(0, 8, body, 0)

    def ring(first, way):
        i = ix if first == "x" else iy
        near = ((x_next, x_prev) if first == "x" else (y_next, y_prev))[way]
        return i, 1 - 2 * way, near

    def launch(st):
        for way in range(2):
            i, sign, near = ring(st.first, way)
            src = st.partial.at[st.chunk(way, mod4(i - sign))]
            wire.put(src, st.recv1.at[way, 0], near, st.send1, st.sem1[0])

    def step1(st, s):
        wire.arrived(st.recv1.at[:, s], st.sem1[s])
        for way in range(2):
            i, sign, near = ring(st.first, way)
            c = mod4(i - (2 + s) * sign)
            for j in range(4):
                own = st.partial[c, way, j] if st.first == "x" else st.partial[j, way, c]
                total = st.recv1[way, s, j].astype(F32) + own.astype(F32)
                st.recv1[way, s, j] = total.astype(BF16)
            if s < 2:
                wire.put(
                    st.recv1.at[way, s], st.recv1.at[way, s + 1], near, st.send1, st.sem1[s + 1]
                )
            else:
                i, sign, near = ring("y" if st.first == "x" else "x", way)
                src = st.recv1.at[way, 2, mod4(i - sign)]
                wire.put(src, st.recv2.at[way, 0], near, st.send2, st.sem2[0])

    def step2(st, s):
        wire.arrived(st.recv2.at[:, s], st.sem2[s])
        for way in range(2):
            i, sign, near = ring("y" if st.first == "x" else "x", way)
            c = mod4(i - (2 + s) * sign)
            total = st.recv2[way, s].astype(F32) + st.recv1[way, 2, c].astype(F32)
            st.recv2[way, s] = total.astype(BF16)
            if s < 2:
                wire.put(
                    st.recv2.at[way, s], st.recv2.at[way, s + 1], near, st.send2, st.sem2[s + 1]
                )
        if s == 2:
            wire.put(st.recv2.at[1 - zh, 2], st.recv3, z_far, st.send3, st.sem3)

    def result(st):
        wire.arrived(st.recv3, st.sem3)
        return (st.recv2[zh, 2].astype(F32) + st.recv3[...].astype(F32)).astype(BF16)

    def row_part(r0):
        def body(n, carry):
            cols = pl.ds(pl.multiple_of(n * 256, 256), 256)
            r = nt(gd[r0 : r0 + 256, :], wg[cols, :]) + nt(ud[r0 : r0 + 256, :], wu[cols, :])
            rg[r0 : r0 + 256, cols] = r.astype(BF16)
            return carry

        lax.fori_loop(0, D // 256, body, 0)

    rc_send, rc_far, rc_near = wire.group(rc), wire.sem(), wire.sem()
    rz_send, rz_in = wire.group(rz), wire.sem()
    cg_send, cg_sem = wire.group(cg_rows.at[pl.ds(1, 3)]), wire.sem()

    for j in range(4):
        pass_dy(j)
        wire.arrived(dy_block(3, j), dy_diag[j])
        down_part(d[j].partial, 512 * j)
        launch(d[j])
        hidden_part(256, j == 0, 512 * j, 512)
        if j == 0:
            turned(256)
        if j == 2:
            step1(d[0], 0)
            step1(d[1], 0)
    backward(256)
    up_part(g0.partial, gd, 0)
    launch(g0)
    up_part(g1.partial, gd, 384)
    launch(g1)
    step1(d[0], 1)
    step1(d[2], 0)
    step1(d[1], 1)
    step1(d[3], 0)
    up_part(u0.partial, ud, 0)
    launch(u0)
    up_part(u1.partial, ud, 384)
    launch(u1)
    step1(d[0], 2)
    step1(d[2], 1)
    step1(d[1], 2)
    step1(d[3], 1)
    row_part(256)
    wire.put(slot_rows(rg, 3), rc.at[1], mate, rc_send, rc_far)
    for slot in range(4):
        row = jnp.sum(jnp.transpose(cg_part[slot * T : slot * T + T, :]), axis=0, keepdims=True)
        cg_rows[slot] = jnp.broadcast_to(row, (8, T))
    for j, to in ((1, mate), (2, z_near), (3, z_diag)):
        wire.put(cg_rows.at[j], cg_in.at[j], to, cg_send, cg_sem)
    step1(g0, 0)
    step1(g1, 0)
    step1(d[2], 2)
    step1(d[3], 2)
    row_part(0)
    wire.put(slot_rows(rg, 1), rc.at[0], mate, rc_send, rc_near)
    step1(u0, 0)
    step1(u1, 0)
    wire.arrived(rc.at[1], rc_far)

    def add_far(i, carry):
        rows = pl.ds(pl.multiple_of(i * 16, 16), 16)
        full = pl.ds(pl.multiple_of(2 * T + i * 16, 16), 16)
        total = rg[full, :].astype(F32) + rc[1, rows, :].astype(F32)
        rg[full, :] = total.astype(BF16)
        return carry

    lax.fori_loop(0, T // 16, add_far, 0)
    wire.put(slot_rows(rg, 2), rz, z_near, rz_send, rz_in)

    step2(d[0], 0)
    step2(d[1], 0)
    step1(g0, 1)
    step1(g1, 1)
    step2(d[2], 0)
    step2(d[3], 0)
    step1(u0, 1)
    step1(u1, 1)

    wire.arrived(cg_in.at[pl.ds(1, 3)], cg_sem)
    answer = jnp.zeros((2, T), F32)
    for j in range(4):
        row = cg_rows[0, 0:1, :] if j == 0 else cg_in[j, 0:1, :]
        answer += jnp.where(ids_ref[...] == jnp.bitwise_xor(ex, j), row, 0.0)
    cg_out[...] = answer
    stores = [pltpu.make_async_copy(cg_out, cg_hbm, local_sem.at[5])]
    stores[0].start()

    for st in d:
        step2(st, 1)
    step1(g0, 2)
    step1(g1, 2)
    for st in d:
        step2(st, 2)
    step1(u0, 2)
    step1(u1, 2)
    step2(g0, 0)
    step2(g1, 0)

    wire.arrived(rc.at[0], rc_near)
    wire.arrived(rz, rz_in)

    def add_rows(i, carry):
        rows = pl.ds(pl.multiple_of(i * 16, 16), 16)
        total = rg[rows, :].astype(F32) + rc[0, rows, :].astype(F32) + rz[rows, :].astype(F32)
        ig_out[rows, :] = total.astype(BF16)
        return carry

    lax.fori_loop(0, T // 16, add_rows, 0)
    stores.append(pltpu.make_async_copy(ig_out, ig_hbm, local_sem.at[6]))
    stores[1].start()

    step2(u0, 0)
    step2(u1, 0)
    step2(g0, 1)
    step2(g1, 1)
    for j in range(4):
        dg_out[0, :, 512 * j : 512 * j + 512] = result(d[j])
    stores.append(pltpu.make_async_copy(dg_out, dg_hbm, local_sem.at[7]))
    stores[2].start()
    step2(u0, 1)
    step2(u1, 1)
    step2(g0, 2)
    step2(g1, 2)
    step2(u0, 2)
    step2(u1, 2)
    gg_out[0, :, 0:384] = result(g0)
    gg_out[0, :, 384:768] = result(g1)
    stores.append(pltpu.make_async_copy(gg_out, gg_hbm, local_sem.at[8]))
    stores[3].start()
    ug_out[0, :, 0:384] = result(u0)
    ug_out[0, :, 384:768] = result(u1)
    stores.append(pltpu.make_async_copy(ug_out, ug_hbm, local_sem.at[9]))
    stores[4].start()

    wire.finish()
    for store in stores:
        store.wait()


def hand_over(*refs):
    for src, dst in zip(refs[:5], refs[5:]):
        dst[...] = src[...]


OUTS = (
    jax.ShapeDtypeStruct((T, D), BF16),
    jax.ShapeDtypeStruct((2, T), F32),
    jax.ShapeDtypeStruct((1, 64, FF), BF16),
    jax.ShapeDtypeStruct((1, 64, FF), BF16),
    jax.ShapeDtypeStruct((1, 24, D), BF16),
)


def shards(tokens, cotangent, expert_ids, combine, w_gate, w_up, w_down):
    hbm = pl.BlockSpec(memory_space=pl.ANY)
    vmem = pl.BlockSpec(memory_space=pltpu.VMEM)
    outs = pl.pallas_call(
        kernel,
        out_shape=OUTS,
        in_specs=[hbm, hbm, vmem, vmem, hbm, hbm, hbm],
        out_specs=(hbm, hbm, hbm, hbm, hbm),
        scratch_shapes=[
            pltpu.VMEM((D, FF), BF16),
            pltpu.VMEM((D, FF), BF16),
            pltpu.VMEM((FF, D), BF16),
            pltpu.VMEM((4 * T, D), BF16),
            pltpu.VMEM((4 * T, D), BF16),
            pltpu.VMEM((D, 4 * T), BF16),
            pltpu.VMEM((256, FF), F32),
            pltpu.VMEM((256, FF), F32),
            pltpu.VMEM((256, FF), F32),
            pltpu.VMEM((256, FF), F32),
            pltpu.VMEM((256, FF), BF16),
            pltpu.VMEM((FF, 4 * T), BF16),
            pltpu.VMEM((4 * T, FF), BF16),
            pltpu.VMEM((4 * T, FF), BF16),
            pltpu.VMEM((4, 8, T), F32),
            pltpu.VMEM((4 * T, T), F32),
            pltpu.VMEM((4 * T, T), F32),
            pltpu.VMEM((4, 8, T), F32),
            pltpu.VMEM((4, 8, T), F32),
            pltpu.VMEM((4 * T, D), BF16),
            pltpu.VMEM((2, T, D), BF16),
            pltpu.VMEM((T, D), BF16),
            pltpu.VMEM((4, 4, 2, 4, 24, 512), BF16),
            pltpu.VMEM((4, 4, 2, 4, 64, 384), BF16),
            pltpu.VMEM((4, 2, 3, 4, 24, 512), BF16),
            pltpu.VMEM((4, 2, 3, 4, 64, 384), BF16),
            pltpu.VMEM((4, 2, 3, 24, 512), BF16),
            pltpu.VMEM((4, 2, 3, 64, 384), BF16),
            pltpu.VMEM((4, 24, 512), BF16),
            pltpu.VMEM((4, 64, 384), BF16),
            pltpu.VMEM((T, D), BF16),
            pltpu.VMEM((2, T), F32),
            pltpu.VMEM((1, 64, FF), BF16),
            pltpu.VMEM((1, 64, FF), BF16),
            pltpu.VMEM((1, 24, D), BF16),
            pltpu.SemaphoreType.DMA((10,)),
            pltpu.SemaphoreType.DMA((N_SEM,)),
        ],
        compiler_params=pltpu.CompilerParams(
            collective_id=0, has_side_effects=True, vmem_limit_bytes=60 * 1024 * 1024
        ),
        name="experts",
    )(tokens, cotangent, expert_ids.T, combine.T, w_gate, w_up, w_down)
    outs = pl.pallas_call(
        hand_over,
        out_shape=OUTS,
        in_specs=[vmem] * 5,
        out_specs=(vmem,) * 5,
        name="hand_over",
    )(*outs)
    return (outs[0], outs[1].T, *outs[2:])


def solution(mesh):
    both = ("dp", "expert")
    return jax.shard_map(
        shards,
        mesh=mesh,
        in_specs=(
            P(both, None),
            P(both, None),
            P(both, None),
            P(both, None),
            P("expert", None, None),
            P("expert", None, None),
            P("expert", None, None),
        ),
        out_specs=(
            P(both, None),
            P(both, None),
            P("expert", "dp", None),
            P("expert", "dp", None),
            P("expert", "dp", None),
        ),
        check_vma=False,
    )
```

```python
import jax
import jax.numpy as jnp
from jax import lax
from jax.experimental import pallas as pl
from jax.experimental.pallas import tpu as pltpu
from jax.sharding import PartitionSpec as P

MESH = pl.DeviceIdType.MESH
BF16 = jnp.bfloat16
F32 = jnp.float32
D = 2048
FF = 768
T = 128
N_SEM = 150


def mod4(v):
    return lax.rem(v + 8, 4)


def nt(a, b):
    return lax.dot_general(a, b, (((1,), (1,)), ((), ())), preferred_element_type=F32)


def nn(a, b):
    return jnp.dot(a, b, preferred_element_type=F32)


class Wire:
    def __init__(self, sems, other):
        self.sems, self.other, self.count, self.groups = sems, other, 0, []

    def sem(self):
        self.count += 1
        return self.sems.at[self.count - 1]

    def describe(self, src, dst, send, recv, device):
        return pltpu.make_async_remote_copy(
            src_ref=src,
            dst_ref=dst,
            send_sem=send,
            recv_sem=recv,
            device_id=device,
            device_id_type=MESH,
        )

    def group(self, total):
        send = self.sem()
        self.groups.append((send, total))
        return send

    def put(self, src, dst, device, send, recv):
        self.describe(src, dst, send, recv, device).start()

    def arrived(self, ref, recv):
        self.describe(ref, ref, recv, recv, self.other).wait_recv()

    def finish(self):
        for send, total in self.groups:
            self.describe(total, total, send, send, self.other).wait_send()


class Sums:
    def __init__(self, right, out, parts, store):
        self.right, self.out, self.parts, self.store = right, out, parts, store

    def put(self, rows, c0, value):
        self.out[0, rows, c0 : c0 + value.shape[1]] = value.astype(BF16)

    def count(self):
        self.parts -= 1
        if self.parts == 0:
            self.store()


class Stream:
    def __init__(self, wire, first, partial, recv1, recv2, recv3, sends, sums, c0, far=False):
        self.first, self.partial, self.far = first, partial, far
        self.second = "y" if first == "x" else "x"
        self.sums, self.c0 = sums, c0
        self.recv1, self.recv2, self.recv3 = recv1, recv2, recv3
        self.send1, self.send2, self.send3 = sends
        self.sem1 = [wire.sem() for _ in range(2)]
        self.sem2 = [wire.sem() for _ in range(2)]
        self.sem3 = wire.sem()

    def chunk(self, way, c):
        if self.far:
            rows = pl.ds(32 * way, 32)
            return (c, slice(None), rows) if self.first == "x" else (slice(None), c, rows)
        return (c, way) if self.first == "x" else (slice(None), way, c)

    def own(self, way, c, j):
        x, y = (c, j) if self.first == "x" else (j, c)
        if self.far:
            return self.recv3[x, y, 32 * way : 32 * way + 32]
        return self.partial[x, way, y]


def kernel(
    x_hbm,
    dy_hbm,
    ids_ref,
    comb_ref,
    wg_hbm,
    wu_hbm,
    wd_hbm,
    ig_hbm,
    cg_hbm,
    gg_hbm,
    ug_hbm,
    dg_hbm,
    wg,
    wu,
    wd,
    x,
    dy,
    xt,
    act,
    dact,
    hid,
    hg,
    hc,
    hct,
    gd,
    ud,
    weight_rows,
    weight_cols,
    cg_part,
    cg_rows,
    cg_in,
    rg,
    rc,
    rz,
    pd,
    pg,
    pz,
    rd1,
    rg1,
    rz1,
    rd2,
    rg2,
    rz2,
    rd3,
    rg3,
    rz3,
    ig_out,
    cg_out,
    gg_out,
    ug_out,
    dg_out,
    local_sem,
    remote_sem,
):
    dp, ex = lax.axis_index("dp"), lax.axis_index("expert")
    ix, zh, iy = lax.div(dp, 8), lax.rem(lax.div(dp, 4), 2), lax.rem(dp, 4)
    zl, core = lax.div(ex, 2), lax.rem(ex, 2)

    def at(a, b, c):
        return {"dp": a * 8 + b * 4 + c, "expert": ex}

    x_next, x_prev = at(mod4(ix + 1), zh, iy), at(mod4(ix - 1), zh, iy)
    y_next, y_prev = at(ix, zh, mod4(iy + 1)), at(ix, zh, mod4(iy - 1))
    z_far = at(ix, 1 - zh, iy)
    mate = {"dp": dp, "expert": zl * 2 + 1 - core}
    z_near = {"dp": dp, "expert": (1 - zl) * 2 + core}
    z_diag = {"dp": dp, "expert": (1 - zl) * 2 + 1 - core}

    loads = [
        pltpu.make_async_copy(x_hbm, x.at[pl.ds(0, T)], local_sem.at[0]),
        pltpu.make_async_copy(dy_hbm, dy.at[pl.ds(0, T)], local_sem.at[1]),
        pltpu.make_async_copy(wg_hbm.at[0], wg, local_sem.at[2]),
        pltpu.make_async_copy(wu_hbm.at[0], wu, local_sem.at[3]),
        pltpu.make_async_copy(wd_hbm.at[0], wd, local_sem.at[4]),
    ]
    for load in loads:
        load.start()

    barrier = pltpu.get_barrier_semaphore()
    peers = (x_next, x_prev, y_next, y_prev, z_far, mate, z_near, z_diag)
    for peer in peers:
        pl.semaphore_signal(barrier, inc=1, device_id=peer, device_id_type=MESH)
    pl.semaphore_wait(barrier, len(peers))

    wire = Wire(remote_sem, mate)

    def slot_rows(ref, slot):
        return ref.at[pl.ds(slot * T, T)]

    def x_block(slot, j):
        return x.at[pl.ds(slot * T + 64 * j, 64)]

    def dy_block(slot, j):
        return dy.at[pl.ds(slot * T, T), pl.ds(256 * j, 256)]

    x_near_send, x_near = wire.group(slot_rows(x, 0)), [wire.sem() for _ in range(2)]
    x_mate_send, x_mate = wire.group(slot_rows(x, 0)), wire.sem()
    x_pass_send, x_diag = wire.group(slot_rows(x, 2)), [wire.sem() for _ in range(2)]
    dy_near_send, dy_near = wire.group(slot_rows(dy, 0)), [wire.sem() for _ in range(8)]
    dy_mate_send, dy_mate = wire.group(slot_rows(dy, 0)), wire.sem()
    dy_pass_send, dy_diag = wire.group(slot_rows(dy, 2)), [wire.sem() for _ in range(8)]
    w_send, w_in = wire.group(weight_rows.at[pl.ds(1, 3)]), wire.sem()

    expert = lax.broadcasted_iota(jnp.int32, (8, T), 0)
    dense = jnp.zeros((8, T), F32)
    for k in range(2):
        dense += jnp.where(ids_ref[k : k + 1, :] == expert, comb_ref[k : k + 1, :], 0.0)
    weight_rows[0] = dense
    for j, to in ((1, mate), (2, z_near), (3, z_diag)):
        wire.put(weight_rows.at[0], weight_rows.at[j], to, w_send, w_in)

    loads[0].wait()
    for j in range(2):
        wire.put(x_block(0, j), x_block(2, j), z_near, x_near_send, x_near[j])
    wire.put(slot_rows(x, 0), slot_rows(x, 1), mate, x_mate_send, x_mate)
    loads[1].wait()
    for j in range(8):
        wire.put(dy_block(0, j), dy_block(2, j), z_near, dy_near_send, dy_near[j])
    wire.put(slot_rows(dy, 0), slot_rows(dy, 1), mate, dy_mate_send, dy_mate)

    def pass_x(j):
        wire.arrived(x_block(2, j), x_near[j])
        wire.put(x_block(2, j), x_block(3, j), mate, x_pass_send, x_diag[j])

    def pass_dy(j):
        wire.arrived(dy_block(2, j), dy_near[j])
        wire.put(dy_block(2, j), dy_block(3, j), mate, dy_pass_send, dy_diag[j])

    def column_weights(slot):
        row = weight_rows[slot, pl.ds(ex, 1), :]
        weight_cols[slot * T : slot * T + T, :] = jnp.transpose(jnp.broadcast_to(row, (T, T)))

    def spread(start):
        col = weight_cols[pl.ds(start, 16), :]
        return jnp.concatenate([col] * 6, axis=1)

    def turned(r0):
        def body(j, carry):
            cols = pl.ds(pl.multiple_of(j * 256, 256), 256)
            xt[cols, r0 : r0 + 256] = jnp.transpose(x[r0 : r0 + 256, cols])
            return carry

        lax.fori_loop(0, D // 256, body, 0)

    def gated(rows, start):
        gate, up = act[rows, :], dact[rows, :]
        s = jax.nn.sigmoid(gate)
        a = gate * s
        h = a * up
        act[rows, :] = a
        dact[rows, :] = up * s * (1.0 + gate * (1.0 - s))
        hid[rows, :] = h
        hc[rows, :] = (h * spread(start)).astype(BF16)

    def hidden_turned(r0):
        def turn(n, carry):
            cols = pl.ds(pl.multiple_of(n * 256, 256), 256)
            hct[cols, r0 : r0 + 256] = jnp.transpose(hc[:, cols])
            return carry

        lax.fori_loop(0, FF // 256, turn, 0)

    def forward():
        def matmul(n, carry):
            cols = pl.ds(pl.multiple_of(n * 256, 256), 256)
            act[:, cols] = nn(x[0:256, :], wg[:, cols])
            dact[:, cols] = nn(x[0:256, :], wu[:, cols])
            return carry

        lax.fori_loop(0, FF // 256, matmul, 0)

        def pointwise(i, carry):
            start = pl.multiple_of(i * 16, 16)
            gated(pl.ds(start, 16), start)
            return carry

        lax.fori_loop(0, 16, pointwise, 0)
        hidden_turned(0)

    def other_matmul(b):
        def matmul(n, carry):
            cols = pl.ds(pl.multiple_of(n * 256, 256), 256)
            starts = (2 * T + 64 * b, 3 * T + 64 * b)
            left = jnp.concatenate([x[r : r + 64, :] for r in starts], axis=0)
            for out, w in ((act, wg), (dact, wu)):
                r = nn(left, w[:, cols])
                out[64 * b : 64 * b + 64, cols] = r[0:64]
                out[T + 64 * b : T + 64 * b + 64, cols] = r[64:128]
            return carry

        lax.fori_loop(0, FF // 256, matmul, 0)

    def other_pointwise(b):
        def pointwise(i, carry):
            start = 64 * b + T * lax.div(i, 4) + 16 * lax.rem(i, 4)
            start = pl.multiple_of(start, 16)
            gated(pl.ds(start, 16), pl.multiple_of(256 + start, 16))
            return carry

        lax.fori_loop(0, 8, pointwise, 0)
        if b == 1:
            hidden_turned(256)

    def hidden_part(r0, first, j0, width):
        def matmul(n, carry):
            cols = pl.ds(pl.multiple_of(n * 256, 256), 256)
            r = nt(dy[r0 : r0 + 256, j0 : j0 + width], wd[cols, j0 : j0 + width])
            hg[:, cols] = r if first else hg[:, cols] + r
            return carry

        lax.fori_loop(0, FF // 256, matmul, 0)

    def backward(r0):
        def pointwise(i, carry):
            rows = pl.ds(pl.multiple_of(i * 16, 16), 16)
            full = pl.ds(pl.multiple_of(r0 + i * 16, 16), 16)
            g = hg[rows, :]
            prod = g * hid[rows, :]
            total = prod[:, 0:128]
            for j in range(1, 6):
                total += prod[:, 128 * j : 128 * j + 128]
            cg_part[full, :] = total
            g = g * spread(pl.multiple_of(r0 + i * 16, 16))
            gd[full, :] = (g * dact[rows, :]).astype(BF16)
            ud[full, :] = (g * act[rows, :]).astype(BF16)
            return carry

        lax.fori_loop(0, 16, pointwise, 0)

    loads[2].wait()
    loads[3].wait()
    wire.arrived(slot_rows(x, 1), x_mate)
    wire.arrived(weight_rows.at[pl.ds(1, 3)], w_in)
    for slot in range(4):
        column_weights(slot)
    forward()
    pass_x(0)
    turned(0)
    loads[4].wait()
    wire.arrived(slot_rows(dy, 1), dy_mate)
    hidden_part(0, True, 0, D)
    backward(0)
    wire.arrived(x_block(3, 0), x_diag[0])
    other_matmul(0)
    pass_x(1)
    other_pointwise(0)
    wire.arrived(x_block(3, 1), x_diag[1])

    stores = []

    def store(src, dst):
        stores.append(pltpu.make_async_copy(src, dst, local_sem.at[5 + len(stores)]))
        stores[-1].start()

    down = Sums(None, dg_out, 8, lambda: store(dg_out, dg_hbm))
    gate = Sums(gd, gg_out, 4, lambda: store(gg_out, gg_hbm))
    upper = Sums(ud, ug_out, 4, lambda: store(ug_out, ug_hbm))
    d_sends = [wire.group(ref) for ref in (rd1, rd2, rd3)]
    g_sends = [wire.group(ref) for ref in (rg1, rg2, rg3)]
    z_sends = [wire.group(ref) for ref in (rz1, rz2, rz3)]
    def axis(j):
        return "xy"[j % 2]

    d = [
        Stream(wire, axis(j), pd.at[j], rd1.at[j], rd2.at[j], rd3.at[j], d_sends, down, 256 * j)
        for j in range(8)
    ]
    up = [
        Stream(wire, axis(j), pg.at[j], rg1.at[j], rg2.at[j], rg3.at[j], g_sends, sums, 256 * (j % 2))
        for j, sums in enumerate((gate, gate, upper, upper))
    ]
    far = [
        Stream(wire, axis(j), pz.at[j], rz1.at[j], rz2.at[j], rz3.at[j], z_sends, sums, c0, True)
        for j, (sums, c0) in enumerate(((gate, 512), (gate, 640), (upper, 512), (upper, 640)))
    ]

    def ring(first, way):
        i = ix if first == "x" else iy
        near = (x_next, x_prev) if first == "x" else (y_next, y_prev)
        return i, 1 - 2 * way, near[way], near[1 - way]

    def launch_relay(st):
        source = st.recv3 if st.far else st.partial
        for way in range(2):
            i, sign, ahead, behind = ring(st.first, way)
            src = source.at[st.chunk(way, mod4(i + 2))]
            wire.put(src, st.recv1.at[way, 0], behind, st.send1, st.sem1[0])

    def launch_direct(st):
        source = st.recv3 if st.far else st.partial
        for way in range(2):
            i, sign, ahead, behind = ring(st.first, way)
            src = source.at[st.chunk(way, mod4(i + sign))]
            wire.put(src, st.recv1.at[way, 1], ahead, st.send1, st.sem1[1])

    def launch(st):
        launch_relay(st)
        launch_direct(st)

    def down_part(j):
        wire.arrived(dy_block(3, j), dy_diag[j])
        r = nn(hct[...], dy[:, 256 * j : 256 * j + 256]).reshape(4, 2, 4, 24, 256)
        pd[j] = r.astype(BF16)
        launch(d[j])

    def up_chunk(st, away):
        right, c0 = st.sums.right, st.c0
        for way in range(2):
            i, sign, ahead, behind = ring(st.first, way)
            c = mod4(i + away * sign)
            if st.first == "x":
                rows = pl.multiple_of(c * 512 + way * 256, 256)
                left = xt[pl.ds(rows, 256), :]
            else:
                starts = [pl.multiple_of(j * 512 + way * 256 + c * 64, 64) for j in range(4)]
                left = jnp.concatenate([xt[pl.ds(r, 64), :] for r in starts], axis=0)
            r = nn(left, right[:, c0 : c0 + 256]).astype(BF16).reshape(4, 64, 256)
            if st.first == "x":
                st.partial[c, way] = r
            else:
                for j in range(4):
                    st.partial[j, way, c] = r[j]

    def up_first(st):
        up_chunk(st, 2)
        launch_relay(st)

    def up_rest(st):
        up_chunk(st, 1)
        launch_direct(st)

        up_chunk(st, -1)
        up_chunk(st, 0)

    def far_part(kind, half):
        right, k = (gd, ud)[kind], 2 * kind

        def body(c, carry):
            rows = pl.multiple_of(c * 512 + half * 256, 256)
            r = nn(xt[pl.ds(rows, 256), :], right[:, 512:768]).astype(BF16)
            r = r.reshape(4, 64, 256)
            pz[k, c, half] = r[:, :, 0:128]
            pz[k + 1, c, half] = r[:, :, 128:256]
            return carry

        lax.fori_loop(0, 4, body, 0)

    def far_first(kind):
        far_part(kind, 1 - zh)
        for st in far[2 * kind : 2 * kind + 2]:
            wire.put(st.partial.at[:, 1 - zh], st.recv3, z_far, st.send3, st.sem3)

    def far_sum(st):
        wire.arrived(st.recv3, st.sem3)

        def body(c, carry):
            for j in range(4):
                total = st.recv3[c, j].astype(F32) + st.partial[c, zh, j].astype(F32)
                st.recv3[c, j] = total.astype(BF16)
            return carry

        lax.fori_loop(0, 4, body, 0)
        launch(st)

    def step1(st, s):
        if s == 0:
            wire.arrived(st.recv1.at[:, 0], st.sem1[0])
        else:
            wire.arrived(st.recv1.at[:, pl.ds(1, 2)], st.sem1[1])
        for way in range(2):
            i, sign, ahead, behind = ring(st.first, way)
            c = mod4(i - sign) if s == 0 else i
            for j in range(4):
                total = st.recv1[way, s, j].astype(F32) + st.own(way, c, j).astype(F32)
                if s == 1:
                    total += st.recv1[way, 2, j].astype(F32)
                st.recv1[way, 2 * s, j] = total.astype(BF16)
            if s == 0:
                wire.put(st.recv1.at[way, 0], st.recv1.at[way, 2], behind, st.send1, st.sem1[1])
        if s == 1:
            for way in range(2):
                i, sign, ahead, behind = ring(st.second, way)
                src = st.recv1.at[way, 2, mod4(i + 2)]
                wire.put(src, st.recv2.at[way, 0], behind, st.send2, st.sem2[0])
            for way in range(2):
                i, sign, ahead, behind = ring(st.second, way)
                src = st.recv1.at[way, 2, mod4(i + sign)]
                wire.put(src, st.recv2.at[way, 1], ahead, st.send2, st.sem2[1])

    def step2(st, s):
        if s == 0:
            wire.arrived(st.recv2.at[:, 0], st.sem2[0])
        else:
            wire.arrived(st.recv2.at[:, pl.ds(1, 2)], st.sem2[1])
        for way in range(2):
            i, sign, ahead, behind = ring(st.second, way)
            c = mod4(i - sign) if s == 0 else i
            total = st.recv2[way, s].astype(F32) + st.recv1[way, 2, c].astype(F32)
            if s == 0:
                st.recv2[way, 0] = total.astype(BF16)
                wire.put(st.recv2.at[way, 0], st.recv2.at[way, 2], behind, st.send2, st.sem2[1])
                continue
            total += st.recv2[way, 2].astype(F32)
            if st.far:
                st.sums.put(slice(32 * way, 32 * way + 32), st.c0, total)
            else:
                st.recv2[way, 2] = total.astype(BF16)
        if s == 1 and st.far:
            st.sums.count()
        elif s == 1:
            wire.put(st.recv2.at[1 - zh, 2], st.recv3, z_far, st.send3, st.sem3)

    def result(st):
        wire.arrived(st.recv3, st.sem3)
        total = st.recv2[zh, 2].astype(F32) + st.recv3[...].astype(F32)
        st.sums.put(slice(None), st.c0, total)
        st.sums.count()

    rc_send, rc_far, rc_near = wire.group(rc), wire.sem(), wire.sem()
    rz_send, rz_in = wire.group(rz), wire.sem()
    cg_send, cg_sem = wire.group(cg_rows.at[pl.ds(1, 3)]), wire.sem()

    def row_part(half, q):
        r0 = 256 * half

        def body(n, carry):
            cols = pl.ds(pl.multiple_of(q * 512 + n * 256, 256), 256)
            r = nt(gd[r0 : r0 + 256, :], wg[cols, :]) + nt(ud[r0 : r0 + 256, :], wu[cols, :])
            rg[r0 : r0 + 256, cols] = r.astype(BF16)
            return carry

        lax.fori_loop(0, 2, body, 0)
        if q == 3:
            if half == 1:
                wire.put(slot_rows(rg, 3), rc.at[1], mate, rc_send, rc_far)
            else:
                wire.put(slot_rows(rg, 1), rc.at[0], mate, rc_send, rc_near)

    def add_far():
        wire.arrived(rc.at[1], rc_far)

        def body(i, carry):
            rows = pl.ds(pl.multiple_of(i * 16, 16), 16)
            full = pl.ds(pl.multiple_of(2 * T + i * 16, 16), 16)
            total = rg[full, :].astype(F32) + rc[1, rows, :].astype(F32)
            rg[full, :] = total.astype(BF16)
            return carry

        lax.fori_loop(0, T // 16, body, 0)
        wire.put(slot_rows(rg, 2), rz, z_near, rz_send, rz_in)

    def add_rows():
        wire.arrived(rc.at[0], rc_near)
        wire.arrived(rz, rz_in)

        def body(i, carry):
            rows = pl.ds(pl.multiple_of(i * 16, 16), 16)
            total = rg[rows, :].astype(F32) + rc[0, rows, :].astype(F32)
            ig_out[rows, :] = (total + rz[rows, :].astype(F32)).astype(BF16)
            return carry

        lax.fori_loop(0, T // 16, body, 0)
        store(ig_out, ig_hbm)

    def combine_part():
        for slot in range(4):
            part = jnp.transpose(cg_part[slot * T : slot * T + T, :])
            cg_rows[slot] = jnp.broadcast_to(jnp.sum(part, axis=0, keepdims=True), (8, T))
        for j, to in ((1, mate), (2, z_near), (3, z_diag)):
            wire.put(cg_rows.at[j], cg_in.at[j], to, cg_send, cg_sem)

    def combine_result():
        wire.arrived(cg_in.at[pl.ds(1, 3)], cg_sem)
        answer = jnp.zeros((2, T), F32)
        for j in range(4):
            row = cg_rows[0, 0:1, :] if j == 0 else cg_in[j, 0:1, :]
            answer += jnp.where(ids_ref[...] == jnp.bitwise_xor(ex, j), row, 0.0)
        cg_out[...] = answer
        store(cg_out, cg_hbm)

    other_matmul(1)
    pass_dy(0)
    pass_dy(1)
    other_pointwise(1)
    turned(256)
    pass_dy(2)
    pass_dy(3)
    down_part(0)
    down_part(1)
    hidden_part(256, True, 0, 512)
    pass_dy(4)
    down_part(2)
    down_part(3)
    pass_dy(5)
    hidden_part(256, False, 512, 512)
    down_part(4)
    pass_dy(6)
    step1(d[0], 0)
    down_part(5)
    pass_dy(7)
    step1(d[1], 0)
    hidden_part(256, False, 1024, 512)
    down_part(6)
    step1(d[2], 0)
    step1(d[3], 0)
    down_part(7)
    hidden_part(256, False, 1536, 512)
    step1(d[4], 0)
    backward(256)
    far_first(0)
    step1(d[5], 0)
    up_first(up[0])
    up_first(up[2])
    up_first(up[3])
    far_first(1)
    step1(d[6], 0)
    step1(d[1], 1)
    up_first(up[1])
    far_part(0, zh)
    step1(d[3], 1)
    up_rest(up[2])
    step1(d[2], 1)
    step1(d[7], 0)
    far_part(1, zh)
    up_rest(up[1])
    step1(d[5], 1)
    up_rest(up[3])
    row_part(1, 0)
    combine_part()
    row_part(1, 1)
    step1(up[3], 0)
    row_part(1, 2)
    far_sum(far[0])
    row_part(1, 3)
    step1(up[2], 0)
    row_part(0, 0)
    step1(up[1], 0)
    row_part(0, 1)
    step2(d[1], 0)
    step2(d[2], 0)
    step2(d[3], 0)
    row_part(0, 2)
    step1(d[7], 1)
    add_far()
    row_part(0, 3)
    up_rest(up[0])
    step1(up[0], 0)
    step1(d[0], 1)
    step1(d[4], 1)
    step1(d[6], 1)
    far_sum(far[1])
    step2(d[5], 0)
    step1(far[0], 0)
    step1(up[2], 1)
    step2(d[1], 1)
    step2(d[3], 1)
    far_sum(far[2])
    step2(d[7], 0)
    step1(up[3], 1)
    step1(up[1], 1)
    step2(d[2], 1)
    step2(d[0], 0)
    step2(d[4], 0)
    step2(d[6], 0)
    far_sum(far[3])
    step1(up[0], 1)
    step1(far[1], 0)
    step2(d[5], 1)
    step1(far[0], 1)
    step2(up[2], 0)
    step1(far[2], 0)
    step2(d[0], 1)
    step2(d[7], 1)
    step2(d[4], 1)
    step2(d[6], 1)
    step2(up[3], 0)
    step1(far[3], 0)
    step2(up[1], 0)
    step2(up[0], 0)
    step1(far[2], 1)
    step1(far[1], 1)
    step2(far[0], 0)
    step2(up[3], 1)
    step2(up[2], 1)
    step1(far[3], 1)
    step2(up[1], 1)
    add_rows()
    step2(up[0], 1)
    combine_result()
    step2(far[2], 0)
    step2(far[1], 0)
    step2(far[0], 1)
    result(d[1])
    result(d[3])
    result(d[2])
    step2(far[3], 0)
    result(d[5])
    result(d[0])
    result(d[7])
    result(d[4])
    result(d[6])
    step2(far[2], 1)
    step2(far[1], 1)
    result(up[3])
    result(up[2])
    result(up[1])
    step2(far[3], 1)
    result(up[0])

    wire.finish()
    for store in stores:
        store.wait()


def hand_over(*refs):
    for src, dst in zip(refs[:5], refs[5:]):
        dst[...] = src[...]


OUTS = (
    jax.ShapeDtypeStruct((T, D), BF16),
    jax.ShapeDtypeStruct((2, T), F32),
    jax.ShapeDtypeStruct((1, 64, FF), BF16),
    jax.ShapeDtypeStruct((1, 64, FF), BF16),
    jax.ShapeDtypeStruct((1, 24, D), BF16),
)


def shards(tokens, cotangent, expert_ids, combine, w_gate, w_up, w_down):
    hbm = pl.BlockSpec(memory_space=pl.ANY)
    vmem = pl.BlockSpec(memory_space=pltpu.VMEM)
    outs = pl.pallas_call(
        kernel,
        out_shape=OUTS,
        in_specs=[hbm, hbm, vmem, vmem, hbm, hbm, hbm],
        out_specs=(hbm, hbm, hbm, hbm, hbm),
        scratch_shapes=[
            pltpu.VMEM((D, FF), BF16),
            pltpu.VMEM((D, FF), BF16),
            pltpu.VMEM((FF, D), BF16),
            pltpu.VMEM((4 * T, D), BF16),
            pltpu.VMEM((4 * T, D), BF16),
            pltpu.VMEM((D, 4 * T), BF16),
            pltpu.VMEM((256, FF), F32),
            pltpu.VMEM((256, FF), F32),
            pltpu.VMEM((256, FF), F32),
            pltpu.VMEM((256, FF), F32),
            pltpu.VMEM((256, FF), BF16),
            pltpu.VMEM((FF, 4 * T), BF16),
            pltpu.VMEM((4 * T, FF), BF16),
            pltpu.VMEM((4 * T, FF), BF16),
            pltpu.VMEM((4, 8, T), F32),
            pltpu.VMEM((4 * T, T), F32),
            pltpu.VMEM((4 * T, T), F32),
            pltpu.VMEM((4, 8, T), F32),
            pltpu.VMEM((4, 8, T), F32),
            pltpu.VMEM((4 * T, D), BF16),
            pltpu.VMEM((2, T, D), BF16),
            pltpu.VMEM((T, D), BF16),
            pltpu.VMEM((8, 4, 2, 4, 24, 256), BF16),
            pltpu.VMEM((4, 4, 2, 4, 64, 256), BF16),
            pltpu.VMEM((4, 4, 2, 4, 64, 128), BF16),
            pltpu.VMEM((8, 2, 3, 4, 24, 256), BF16),
            pltpu.VMEM((4, 2, 3, 4, 64, 256), BF16),
            pltpu.VMEM((4, 2, 3, 4, 32, 128), BF16),
            pltpu.VMEM((8, 2, 3, 24, 256), BF16),
            pltpu.VMEM((4, 2, 3, 64, 256), BF16),
            pltpu.VMEM((4, 2, 3, 32, 128), BF16),
            pltpu.VMEM((8, 24, 256), BF16),
            pltpu.VMEM((4, 64, 256), BF16),
            pltpu.VMEM((4, 4, 4, 64, 128), BF16),
            pltpu.VMEM((T, D), BF16),
            pltpu.VMEM((2, T), F32),
            pltpu.VMEM((1, 64, FF), BF16),
            pltpu.VMEM((1, 64, FF), BF16),
            pltpu.VMEM((1, 24, D), BF16),
            pltpu.SemaphoreType.DMA((10,)),
            pltpu.SemaphoreType.DMA((N_SEM,)),
        ],
        compiler_params=pltpu.CompilerParams(
            collective_id=0, has_side_effects=True, vmem_limit_bytes=60 * 1024 * 1024
        ),
        name="experts",
    )(tokens, cotangent, expert_ids.T, combine.T, w_gate, w_up, w_down)
    outs = pl.pallas_call(
        hand_over,
        out_shape=OUTS,
        in_specs=[vmem] * 5,
        out_specs=(vmem,) * 5,
        name="hand_over",
    )(*outs)
    return (outs[0], outs[1].T, *outs[2:])


def solution(mesh):
    both = ("dp", "expert")
    return jax.shard_map(
        shards,
        mesh=mesh,
        in_specs=(
            P(both, None),
            P(both, None),
            P(both, None),
            P(both, None),
            P("expert", None, None),
            P("expert", None, None),
            P("expert", None, None),
        ),
        out_specs=(
            P(both, None),
            P(both, None),
            P("expert", "dp", None),
            P("expert", "dp", None),
            P("expert", "dp", None),
        ),
        check_vma=False,
    )
```

```python
import jax
import jax.numpy as jnp
from jax import lax
from jax.experimental import pallas as pl
from jax.experimental.pallas import tpu as pltpu
from jax.sharding import PartitionSpec as P

MESH = pl.DeviceIdType.MESH
BF16 = jnp.bfloat16
F32 = jnp.float32
D = 2048
FF = 768
T = 128
N_SEM = 150


def mod4(v):
    return lax.rem(v + 8, 4)


def nt(a, b):
    return lax.dot_general(a, b, (((1,), (1,)), ((), ())), preferred_element_type=F32)


def nn(a, b):
    return jnp.dot(a, b, preferred_element_type=F32)


class Wire:
    def __init__(self, sems, other):
        self.sems, self.other, self.count, self.groups = sems, other, 0, []

    def sem(self):
        self.count += 1
        return self.sems.at[self.count - 1]

    def describe(self, src, dst, send, recv, device):
        return pltpu.make_async_remote_copy(
            src_ref=src,
            dst_ref=dst,
            send_sem=send,
            recv_sem=recv,
            device_id=device,
            device_id_type=MESH,
        )

    def group(self, total):
        send = self.sem()
        self.groups.append((send, total))
        return send

    def put(self, src, dst, device, send, recv):
        self.describe(src, dst, send, recv, device).start()

    def arrived(self, ref, recv):
        self.describe(ref, ref, recv, recv, self.other).wait_recv()

    def finish(self):
        for send, total in self.groups:
            self.describe(total, total, send, send, self.other).wait_send()


class Sums:
    def __init__(self, right, out):
        self.right, self.out = right, out

    def put(self, rows, c0, value):
        self.out[0, rows, c0 : c0 + value.shape[1]] = value.astype(BF16)


class Stream:
    def __init__(self, wire, first, partial, recv1, recv2, recv3, sends, sums, c0, far=False):
        self.first, self.partial, self.far = first, partial, far
        self.second = "y" if first == "x" else "x"
        self.sums, self.c0 = sums, c0
        self.recv1, self.recv2, self.recv3 = recv1, recv2, recv3
        self.send1, self.send2, self.send3 = sends
        self.sem1 = [wire.sem() for _ in range(2)]
        self.sem2 = [wire.sem() for _ in range(2)]
        self.sem3 = wire.sem()

    def chunk(self, way, c):
        if self.far:
            rows = pl.ds(32 * way, 32)
            return (c, slice(None), rows) if self.first == "x" else (slice(None), c, rows)
        return (c, way) if self.first == "x" else (slice(None), way, c)

    def own(self, way, c, j):
        x, y = (c, j) if self.first == "x" else (j, c)
        if self.far:
            return self.recv3[x, y, 32 * way : 32 * way + 32]
        return self.partial[x, way, y]


def kernel(
    x_hbm,
    dy_hbm,
    ids_ref,
    comb_ref,
    wg_hbm,
    wu_hbm,
    wd_hbm,
    ig_out,
    cg_out,
    gg_out,
    ug_out,
    dg_out,
    wg,
    wu,
    wd,
    x,
    dy,
    xt,
    act,
    dact,
    hid,
    hg,
    hc,
    hct,
    gd,
    ud,
    weight_rows,
    weight_cols,
    cg_part,
    cg_rows,
    cg_in,
    rg,
    rc,
    rz,
    pd,
    pg,
    pz,
    rd1,
    rg1,
    rz1,
    rd2,
    rg2,
    rz2,
    rd3,
    rg3,
    rz3,
    local_sem,
    remote_sem,
):
    dp, ex = lax.axis_index("dp"), lax.axis_index("expert")
    ix, zh, iy = lax.div(dp, 8), lax.rem(lax.div(dp, 4), 2), lax.rem(dp, 4)
    zl, core = lax.div(ex, 2), lax.rem(ex, 2)

    def at(a, b, c):
        return {"dp": a * 8 + b * 4 + c, "expert": ex}

    x_next, x_prev = at(mod4(ix + 1), zh, iy), at(mod4(ix - 1), zh, iy)
    y_next, y_prev = at(ix, zh, mod4(iy + 1)), at(ix, zh, mod4(iy - 1))
    z_far = at(ix, 1 - zh, iy)
    mate = {"dp": dp, "expert": zl * 2 + 1 - core}
    z_near = {"dp": dp, "expert": (1 - zl) * 2 + core}
    z_diag = {"dp": dp, "expert": (1 - zl) * 2 + 1 - core}

    loads = [
        pltpu.make_async_copy(x_hbm, x.at[pl.ds(0, T)], local_sem.at[0]),
        pltpu.make_async_copy(dy_hbm, dy.at[pl.ds(0, T)], local_sem.at[1]),
        pltpu.make_async_copy(wg_hbm.at[0], wg, local_sem.at[2]),
        pltpu.make_async_copy(wu_hbm.at[0], wu, local_sem.at[3]),
        pltpu.make_async_copy(wd_hbm.at[0], wd, local_sem.at[4]),
    ]
    for load in loads:
        load.start()

    barrier = pltpu.get_barrier_semaphore()
    peers = (x_next, x_prev, y_next, y_prev, z_far, mate, z_near, z_diag)
    for peer in peers:
        pl.semaphore_signal(barrier, inc=1, device_id=peer, device_id_type=MESH)
    pl.semaphore_wait(barrier, len(peers))

    wire = Wire(remote_sem, mate)

    def slot_rows(ref, slot):
        return ref.at[pl.ds(slot * T, T)]

    def x_block(slot, j):
        return x.at[pl.ds(slot * T + 64 * j, 64)]

    def dy_block(slot, j):
        return dy.at[pl.ds(slot * T, T), pl.ds(256 * j, 256)]

    x_near_send, x_near = wire.group(slot_rows(x, 0)), [wire.sem() for _ in range(2)]
    x_mate_send, x_mate = wire.group(slot_rows(x, 0)), wire.sem()
    x_pass_send, x_diag = wire.group(slot_rows(x, 2)), [wire.sem() for _ in range(2)]
    dy_near_send, dy_near = wire.group(slot_rows(dy, 0)), [wire.sem() for _ in range(8)]
    dy_mate_send, dy_mate = wire.group(slot_rows(dy, 0)), wire.sem()
    dy_pass_send, dy_diag = wire.group(slot_rows(dy, 2)), [wire.sem() for _ in range(8)]
    w_send, w_in = wire.group(weight_rows.at[pl.ds(1, 3)]), wire.sem()

    expert = lax.broadcasted_iota(jnp.int32, (8, T), 0)
    dense = jnp.zeros((8, T), F32)
    for k in range(2):
        dense += jnp.where(ids_ref[k : k + 1, :] == expert, comb_ref[k : k + 1, :], 0.0)
    weight_rows[0] = dense
    for j, to in ((1, mate), (2, z_near), (3, z_diag)):
        wire.put(weight_rows.at[0], weight_rows.at[j], to, w_send, w_in)

    loads[0].wait()
    for j in range(2):
        wire.put(x_block(0, j), x_block(2, j), z_near, x_near_send, x_near[j])
    wire.put(slot_rows(x, 0), slot_rows(x, 1), mate, x_mate_send, x_mate)
    loads[1].wait()
    for j in range(8):
        wire.put(dy_block(0, j), dy_block(2, j), z_near, dy_near_send, dy_near[j])
    wire.put(slot_rows(dy, 0), slot_rows(dy, 1), mate, dy_mate_send, dy_mate)

    def pass_x(j):
        wire.arrived(x_block(2, j), x_near[j])
        wire.put(x_block(2, j), x_block(3, j), mate, x_pass_send, x_diag[j])

    def pass_dy(j):
        wire.arrived(dy_block(2, j), dy_near[j])
        wire.put(dy_block(2, j), dy_block(3, j), mate, dy_pass_send, dy_diag[j])

    def column_weights(slot):
        row = weight_rows[slot, pl.ds(ex, 1), :]
        weight_cols[slot * T : slot * T + T, :] = jnp.transpose(jnp.broadcast_to(row, (T, T)))

    def spread(start):
        col = weight_cols[pl.ds(start, 16), :]
        return jnp.concatenate([col] * 6, axis=1)

    def turned(r0):
        def body(j, carry):
            cols = pl.ds(pl.multiple_of(j * 256, 256), 256)
            xt[cols, r0 : r0 + 256] = jnp.transpose(x[r0 : r0 + 256, cols])
            return carry

        lax.fori_loop(0, D // 256, body, 0)

    def gated(rows, start):
        gate, up = act[rows, :], dact[rows, :]
        s = jax.nn.sigmoid(gate)
        a = gate * s
        h = a * up
        act[rows, :] = a
        dact[rows, :] = up * s * (1.0 + gate * (1.0 - s))
        hid[rows, :] = h
        hc[rows, :] = (h * spread(start)).astype(BF16)

    def hidden_turned(r0):
        def turn(n, carry):
            cols = pl.ds(pl.multiple_of(n * 256, 256), 256)
            hct[cols, r0 : r0 + 256] = jnp.transpose(hc[:, cols])
            return carry

        lax.fori_loop(0, FF // 256, turn, 0)

    def forward():
        def matmul(n, carry):
            cols = pl.ds(pl.multiple_of(n * 256, 256), 256)
            act[:, cols] = nn(x[0:256, :], wg[:, cols])
            dact[:, cols] = nn(x[0:256, :], wu[:, cols])
            return carry

        lax.fori_loop(0, FF // 256, matmul, 0)

        def pointwise(i, carry):
            start = pl.multiple_of(i * 16, 16)
            gated(pl.ds(start, 16), start)
            return carry

        lax.fori_loop(0, 16, pointwise, 0)
        hidden_turned(0)

    def other_matmul(b):
        def matmul(n, carry):
            cols = pl.ds(pl.multiple_of(n * 256, 256), 256)
            starts = (2 * T + 64 * b, 3 * T + 64 * b)
            left = jnp.concatenate([x[r : r + 64, :] for r in starts], axis=0)
            for out, w in ((act, wg), (dact, wu)):
                r = nn(left, w[:, cols])
                out[64 * b : 64 * b + 64, cols] = r[0:64]
                out[T + 64 * b : T + 64 * b + 64, cols] = r[64:128]
            return carry

        lax.fori_loop(0, FF // 256, matmul, 0)

    def other_pointwise(b):
        def pointwise(i, carry):
            start = 64 * b + T * lax.div(i, 4) + 16 * lax.rem(i, 4)
            start = pl.multiple_of(start, 16)
            gated(pl.ds(start, 16), pl.multiple_of(256 + start, 16))
            return carry

        lax.fori_loop(0, 8, pointwise, 0)
        if b == 1:
            hidden_turned(256)

    def hidden_part(r0, first, j0, width):
        def matmul(n, carry):
            cols = pl.ds(pl.multiple_of(n * 256, 256), 256)
            r = nt(dy[r0 : r0 + 256, j0 : j0 + width], wd[cols, j0 : j0 + width])
            hg[:, cols] = r if first else hg[:, cols] + r
            return carry

        lax.fori_loop(0, FF // 256, matmul, 0)

    def backward(r0):
        def pointwise(i, carry):
            rows = pl.ds(pl.multiple_of(i * 16, 16), 16)
            full = pl.ds(pl.multiple_of(r0 + i * 16, 16), 16)
            g = hg[rows, :]
            prod = g * hid[rows, :]
            total = prod[:, 0:128]
            for j in range(1, 6):
                total += prod[:, 128 * j : 128 * j + 128]
            cg_part[full, :] = total
            g = g * spread(pl.multiple_of(r0 + i * 16, 16))
            gd[full, :] = (g * dact[rows, :]).astype(BF16)
            ud[full, :] = (g * act[rows, :]).astype(BF16)
            return carry

        lax.fori_loop(0, 16, pointwise, 0)

    loads[2].wait()
    loads[3].wait()
    wire.arrived(slot_rows(x, 1), x_mate)
    wire.arrived(weight_rows.at[pl.ds(1, 3)], w_in)
    for slot in range(4):
        column_weights(slot)
    forward()
    pass_x(0)
    turned(0)
    loads[4].wait()
    wire.arrived(slot_rows(dy, 1), dy_mate)
    hidden_part(0, True, 0, D)
    backward(0)
    wire.arrived(x_block(3, 0), x_diag[0])
    other_matmul(0)
    pass_x(1)
    other_pointwise(0)
    pass_dy(0)
    wire.arrived(x_block(3, 1), x_diag[1])

    down = Sums(None, dg_out)
    gate = Sums(gd, gg_out)
    upper = Sums(ud, ug_out)
    d_sends = [wire.group(ref) for ref in (rd1, rd2, rd3)]
    g_sends = [wire.group(ref) for ref in (rg1, rg2, rg3)]
    z_sends = [wire.group(ref) for ref in (rz1, rz2, rz3)]
    def axis(j):
        return "xy"[j % 2]

    d = [
        Stream(wire, axis(j), pd.at[j], rd1.at[j], rd2.at[j], rd3.at[j], d_sends, down, 256 * j)
        for j in range(8)
    ]
    up = [
        Stream(wire, axis(j), pg.at[j], rg1.at[j], rg2.at[j], rg3.at[j], g_sends, sums, 256 * (j % 2))
        for j, sums in enumerate((gate, gate, upper, upper))
    ]
    far = [
        Stream(wire, axis(j), pz.at[j], rz1.at[j], rz2.at[j], rz3.at[j], z_sends, sums, c0, True)
        for j, (sums, c0) in enumerate(((gate, 512), (gate, 640), (upper, 512), (upper, 640)))
    ]

    def ring(first, way):
        i = ix if first == "x" else iy
        near = (x_next, x_prev) if first == "x" else (y_next, y_prev)
        return i, 1 - 2 * way, near[way], near[1 - way]

    def launch_relay(st):
        source = st.recv3 if st.far else st.partial
        for way in range(2):
            i, sign, ahead, behind = ring(st.first, way)
            src = source.at[st.chunk(way, mod4(i + 2))]
            wire.put(src, st.recv1.at[way, 0], behind, st.send1, st.sem1[0])

    def launch_direct(st):
        source = st.recv3 if st.far else st.partial
        for way in range(2):
            i, sign, ahead, behind = ring(st.first, way)
            src = source.at[st.chunk(way, mod4(i + sign))]
            wire.put(src, st.recv1.at[way, 1], ahead, st.send1, st.sem1[1])

    def launch(st):
        launch_relay(st)
        launch_direct(st)

    def down_part(j):
        wire.arrived(dy_block(3, j), dy_diag[j])
        r = nn(hct[...], dy[:, 256 * j : 256 * j + 256]).reshape(4, 2, 4, 24, 256)
        pd[j] = r.astype(BF16)
        launch(d[j])

    def up_chunk(st, away):
        right, c0 = st.sums.right, st.c0
        for way in range(2):
            i, sign, ahead, behind = ring(st.first, way)
            c = mod4(i + away * sign)
            if st.first == "x":
                rows = pl.multiple_of(c * 512 + way * 256, 256)
                left = xt[pl.ds(rows, 256), :]
            else:
                starts = [pl.multiple_of(j * 512 + way * 256 + c * 64, 64) for j in range(4)]
                left = jnp.concatenate([xt[pl.ds(r, 64), :] for r in starts], axis=0)
            r = nn(left, right[:, c0 : c0 + 256]).astype(BF16).reshape(4, 64, 256)
            if st.first == "x":
                st.partial[c, way] = r
            else:
                for j in range(4):
                    st.partial[j, way, c] = r[j]

    def up_first(st):
        up_chunk(st, 2)
        launch_relay(st)

    def up_rest(st):
        up_chunk(st, 1)
        launch_direct(st)

        up_chunk(st, -1)
        up_chunk(st, 0)

    def far_part(kind, half):
        right, k = (gd, ud)[kind], 2 * kind

        def body(c, carry):
            rows = pl.multiple_of(c * 512 + half * 256, 256)
            r = nn(xt[pl.ds(rows, 256), :], right[:, 512:768]).astype(BF16)
            r = r.reshape(4, 64, 256)
            pz[k, c, half] = r[:, :, 0:128]
            pz[k + 1, c, half] = r[:, :, 128:256]
            return carry

        lax.fori_loop(0, 4, body, 0)

    def far_first(kind):
        far_part(kind, 1 - zh)
        for st in far[2 * kind : 2 * kind + 2]:
            wire.put(st.partial.at[:, 1 - zh], st.recv3, z_far, st.send3, st.sem3)

    def far_sum(st):
        wire.arrived(st.recv3, st.sem3)

        def body(c, carry):
            for j in range(4):
                total = st.recv3[c, j].astype(F32) + st.partial[c, zh, j].astype(F32)
                st.recv3[c, j] = total.astype(BF16)
            return carry

        lax.fori_loop(0, 4, body, 0)
        launch(st)

    def step1(st, s):
        if s == 0:
            wire.arrived(st.recv1.at[:, 0], st.sem1[0])
        else:
            wire.arrived(st.recv1.at[:, pl.ds(1, 2)], st.sem1[1])
        for way in range(2):
            i, sign, ahead, behind = ring(st.first, way)
            c = mod4(i - sign) if s == 0 else i
            for j in range(4):
                total = st.recv1[way, s, j].astype(F32) + st.own(way, c, j).astype(F32)
                if s == 1:
                    total += st.recv1[way, 2, j].astype(F32)
                st.recv1[way, 2 * s, j] = total.astype(BF16)
            if s == 0:
                wire.put(st.recv1.at[way, 0], st.recv1.at[way, 2], behind, st.send1, st.sem1[1])
        if s == 1:
            for way in range(2):
                i, sign, ahead, behind = ring(st.second, way)
                src = st.recv1.at[way, 2, mod4(i + 2)]
                wire.put(src, st.recv2.at[way, 0], behind, st.send2, st.sem2[0])
            for way in range(2):
                i, sign, ahead, behind = ring(st.second, way)
                src = st.recv1.at[way, 2, mod4(i + sign)]
                wire.put(src, st.recv2.at[way, 1], ahead, st.send2, st.sem2[1])

    def step2(st, s):
        if s == 0:
            wire.arrived(st.recv2.at[:, 0], st.sem2[0])
        else:
            wire.arrived(st.recv2.at[:, pl.ds(1, 2)], st.sem2[1])
        for way in range(2):
            i, sign, ahead, behind = ring(st.second, way)
            c = mod4(i - sign) if s == 0 else i
            total = st.recv2[way, s].astype(F32) + st.recv1[way, 2, c].astype(F32)
            if s == 0:
                st.recv2[way, 0] = total.astype(BF16)
                wire.put(st.recv2.at[way, 0], st.recv2.at[way, 2], behind, st.send2, st.sem2[1])
                continue
            total += st.recv2[way, 2].astype(F32)
            if st.far:
                st.sums.put(slice(32 * way, 32 * way + 32), st.c0, total)
            else:
                st.recv2[way, 2] = total.astype(BF16)
        if s == 1 and not st.far:
            wire.put(st.recv2.at[1 - zh, 2], st.recv3, z_far, st.send3, st.sem3)

    def result(st):
        wire.arrived(st.recv3, st.sem3)
        total = st.recv2[zh, 2].astype(F32) + st.recv3[...].astype(F32)
        st.sums.put(slice(None), st.c0, total)

    rc_send, rc_far, rc_near = wire.group(rc), wire.sem(), wire.sem()
    rz_send, rz_in = wire.group(rz), wire.sem()
    cg_send, cg_sem = wire.group(cg_rows.at[pl.ds(1, 3)]), wire.sem()

    def row_part(half, q):
        r0 = 256 * half

        def body(n, carry):
            cols = pl.ds(pl.multiple_of(q * 512 + n * 256, 256), 256)
            r = nt(gd[r0 : r0 + 256, :], wg[cols, :]) + nt(ud[r0 : r0 + 256, :], wu[cols, :])
            rg[r0 : r0 + 256, cols] = r.astype(BF16)
            return carry

        lax.fori_loop(0, 2, body, 0)
        if q == 3:
            if half == 1:
                wire.put(slot_rows(rg, 3), rc.at[1], mate, rc_send, rc_far)
            else:
                wire.put(slot_rows(rg, 1), rc.at[0], mate, rc_send, rc_near)

    def add_far():
        wire.arrived(rc.at[1], rc_far)

        def body(i, carry):
            rows = pl.ds(pl.multiple_of(i * 16, 16), 16)
            full = pl.ds(pl.multiple_of(2 * T + i * 16, 16), 16)
            total = rg[full, :].astype(F32) + rc[1, rows, :].astype(F32)
            rg[full, :] = total.astype(BF16)
            return carry

        lax.fori_loop(0, T // 16, body, 0)
        wire.put(slot_rows(rg, 2), rz, z_near, rz_send, rz_in)

    def add_rows():
        wire.arrived(rc.at[0], rc_near)
        wire.arrived(rz, rz_in)

        def body(i, carry):
            rows = pl.ds(pl.multiple_of(i * 16, 16), 16)
            total = rg[rows, :].astype(F32) + rc[0, rows, :].astype(F32)
            ig_out[rows, :] = (total + rz[rows, :].astype(F32)).astype(BF16)
            return carry

        lax.fori_loop(0, T // 16, body, 0)

    def combine_part():
        for slot in range(4):
            part = jnp.transpose(cg_part[slot * T : slot * T + T, :])
            cg_rows[slot] = jnp.broadcast_to(jnp.sum(part, axis=0, keepdims=True), (8, T))
        for j, to in ((1, mate), (2, z_near), (3, z_diag)):
            wire.put(cg_rows.at[j], cg_in.at[j], to, cg_send, cg_sem)

    def combine_result():
        wire.arrived(cg_in.at[pl.ds(1, 3)], cg_sem)
        answer = jnp.zeros((2, T), F32)
        for j in range(4):
            row = cg_rows[0, 0:1, :] if j == 0 else cg_in[j, 0:1, :]
            answer += jnp.where(ids_ref[...] == jnp.bitwise_xor(ex, j), row, 0.0)
        cg_out[...] = answer

    other_matmul(1)
    pass_dy(1)
    other_pointwise(1)
    down_part(0)
    pass_dy(2)
    turned(256)
    pass_dy(3)
    down_part(1)
    hidden_part(256, True, 0, 512)
    pass_dy(4)
    down_part(2)
    down_part(3)
    pass_dy(5)
    hidden_part(256, False, 512, 512)
    step1(d[0], 0)
    down_part(4)
    pass_dy(6)
    step1(d[1], 0)
    down_part(5)
    pass_dy(7)
    hidden_part(256, False, 1024, 512)
    step1(d[2], 0)
    down_part(6)
    step1(d[3], 0)
    down_part(7)
    hidden_part(256, False, 1536, 512)
    step1(d[0], 1)
    backward(256)
    step1(d[1], 1)
    step1(d[4], 0)
    far_first(0)
    step1(d[5], 0)
    far_first(1)
    up_first(up[0])
    step1(d[2], 1)
    up_first(up[1])
    up_first(up[2])
    step1(d[3], 1)
    up_first(up[3])
    step1(d[6], 0)
    far_part(0, zh)
    step1(d[7], 0)
    far_part(1, zh)
    step2(d[1], 0)
    up_rest(up[0])
    step1(d[4], 1)
    step2(d[0], 0)
    up_rest(up[1])
    step1(d[5], 1)
    step2(d[2], 0)
    up_rest(up[2])
    up_rest(up[3])
    step1(up[0], 0)
    combine_part()
    row_part(1, 0)
    step1(up[1], 0)
    row_part(1, 1)
    far_sum(far[0])
    row_part(1, 2)
    step1(up[2], 0)
    step2(d[3], 0)
    row_part(1, 3)
    step1(up[3], 0)
    row_part(0, 0)
    step1(d[6], 1)
    step1(d[7], 1)
    step2(d[1], 1)
    row_part(0, 1)
    step2(d[4], 0)
    step2(d[0], 1)
    row_part(0, 2)
    add_far()
    row_part(0, 3)
    far_sum(far[1])
    step2(d[5], 0)
    step2(d[2], 1)
    far_sum(far[2])
    step1(up[0], 1)
    step1(far[0], 0)
    step1(up[1], 1)
    step1(up[3], 1)
    step2(d[6], 0)
    step1(up[2], 1)
    step2(d[3], 1)
    step2(d[4], 1)
    step2(d[7], 0)
    far_sum(far[3])
    step2(d[5], 1)
    result(d[1])
    step1(far[1], 0)
    result(d[0])
    step1(far[2], 0)
    step2(up[0], 0)
    step1(far[0], 1)
    step2(d[6], 1)
    step2(up[1], 0)
    step2(up[2], 0)
    step2(up[3], 0)
    step1(far[3], 0)
    step2(d[7], 1)
    step1(far[2], 1)
    step1(far[1], 1)
    step2(up[0], 1)
    step2(up[1], 1)
    step2(far[0], 0)
    step2(up[2], 1)
    step2(up[3], 1)
    step1(far[3], 1)
    step2(far[2], 0)
    step2(far[1], 0)
    add_rows()
    combine_result()
    step2(far[0], 1)
    result(d[2])
    step2(far[3], 0)
    result(d[3])
    result(d[4])
    result(d[5])
    step2(far[2], 1)
    step2(far[1], 1)
    result(d[6])
    result(d[7])
    result(up[0])
    result(up[1])
    result(up[2])
    step2(far[3], 1)
    result(up[3])

    wire.finish()


def hand_over(*refs):
    for src, dst in zip(refs[:5], refs[5:]):
        dst[...] = src[...]


OUTS = (
    jax.ShapeDtypeStruct((T, D), BF16),
    jax.ShapeDtypeStruct((2, T), F32),
    jax.ShapeDtypeStruct((1, 64, FF), BF16),
    jax.ShapeDtypeStruct((1, 64, FF), BF16),
    jax.ShapeDtypeStruct((1, 24, D), BF16),
)


def shards(tokens, cotangent, expert_ids, combine, w_gate, w_up, w_down):
    hbm = pl.BlockSpec(memory_space=pl.ANY)
    vmem = pl.BlockSpec(memory_space=pltpu.VMEM)
    outs = pl.pallas_call(
        kernel,
        out_shape=tuple(pltpu.VMEM(o.shape, o.dtype) for o in OUTS),
        in_specs=[hbm, hbm, vmem, vmem, hbm, hbm, hbm],
        out_specs=(vmem,) * 5,
        scratch_shapes=[
            pltpu.VMEM((D, FF), BF16),
            pltpu.VMEM((D, FF), BF16),
            pltpu.VMEM((FF, D), BF16),
            pltpu.VMEM((4 * T, D), BF16),
            pltpu.VMEM((4 * T, D), BF16),
            pltpu.VMEM((D, 4 * T), BF16),
            pltpu.VMEM((256, FF), F32),
            pltpu.VMEM((256, FF), F32),
            pltpu.VMEM((256, FF), F32),
            pltpu.VMEM((256, FF), F32),
            pltpu.VMEM((256, FF), BF16),
            pltpu.VMEM((FF, 4 * T), BF16),
            pltpu.VMEM((4 * T, FF), BF16),
            pltpu.VMEM((4 * T, FF), BF16),
            pltpu.VMEM((4, 8, T), F32),
            pltpu.VMEM((4 * T, T), F32),
            pltpu.VMEM((4 * T, T), F32),
            pltpu.VMEM((4, 8, T), F32),
            pltpu.VMEM((4, 8, T), F32),
            pltpu.VMEM((4 * T, D), BF16),
            pltpu.VMEM((2, T, D), BF16),
            pltpu.VMEM((T, D), BF16),
            pltpu.VMEM((8, 4, 2, 4, 24, 256), BF16),
            pltpu.VMEM((4, 4, 2, 4, 64, 256), BF16),
            pltpu.VMEM((4, 4, 2, 4, 64, 128), BF16),
            pltpu.VMEM((8, 2, 3, 4, 24, 256), BF16),
            pltpu.VMEM((4, 2, 3, 4, 64, 256), BF16),
            pltpu.VMEM((4, 2, 3, 4, 32, 128), BF16),
            pltpu.VMEM((8, 2, 3, 24, 256), BF16),
            pltpu.VMEM((4, 2, 3, 64, 256), BF16),
            pltpu.VMEM((4, 2, 3, 32, 128), BF16),
            pltpu.VMEM((8, 24, 256), BF16),
            pltpu.VMEM((4, 64, 256), BF16),
            pltpu.VMEM((4, 4, 4, 64, 128), BF16),
            pltpu.SemaphoreType.DMA((5,)),
            pltpu.SemaphoreType.DMA((N_SEM,)),
        ],
        compiler_params=pltpu.CompilerParams(
            collective_id=0, has_side_effects=True, vmem_limit_bytes=60 * 1024 * 1024
        ),
        name="experts",
    )(tokens, cotangent, expert_ids.T, combine.T, w_gate, w_up, w_down)
    outs = pl.pallas_call(
        hand_over,
        out_shape=OUTS,
        in_specs=[vmem] * 5,
        out_specs=(vmem,) * 5,
        name="hand_over",
    )(*(pltpu.with_memory_space_constraint(o, pltpu.VMEM) for o in outs))
    return (outs[0], outs[1].T, *outs[2:])


def solution(mesh):
    both = ("dp", "expert")
    return jax.shard_map(
        shards,
        mesh=mesh,
        in_specs=(
            P(both, None),
            P(both, None),
            P(both, None),
            P(both, None),
            P("expert", None, None),
            P("expert", None, None),
            P("expert", None, None),
        ),
        out_specs=(
            P(both, None),
            P(both, None),
            P("expert", "dp", None),
            P("expert", "dp", None),
            P("expert", "dp", None),
        ),
        check_vma=False,
    )
```

```python
import jax
import jax.numpy as jnp
from jax import lax
from jax.experimental import pallas as pl
from jax.experimental.pallas import tpu as pltpu
from jax.sharding import PartitionSpec as P

MESH = pl.DeviceIdType.MESH
BF16 = jnp.bfloat16
F32 = jnp.float32
D = 2048
FF = 768
T = 128
N_SEM = 132


def mod4(v):
    return lax.rem(v + 8, 4)


def nt(a, b):
    return lax.dot_general(a, b, (((1,), (1,)), ((), ())), preferred_element_type=F32)


def nn(a, b):
    return jnp.dot(a, b, preferred_element_type=F32)


class Wire:
    def __init__(self, sems, other):
        self.sems, self.other, self.count, self.groups = sems, other, 0, []

    def sem(self):
        self.count += 1
        return self.sems.at[self.count - 1]

    def describe(self, src, dst, send, recv, device):
        return pltpu.make_async_remote_copy(
            src_ref=src,
            dst_ref=dst,
            send_sem=send,
            recv_sem=recv,
            device_id=device,
            device_id_type=MESH,
        )

    def group(self, total):
        send = self.sem()
        self.groups.append((send, total))
        return send

    def put(self, src, dst, device, send, recv):
        self.describe(src, dst, send, recv, device).start()

    def arrived(self, ref, recv):
        self.describe(ref, ref, recv, recv, self.other).wait_recv()

    def finish(self):
        for send, total in self.groups:
            self.describe(total, total, send, send, self.other).wait_send()


class Sums:
    def __init__(self, right, out):
        self.right, self.out = right, out

    def put(self, rows, c0, value):
        self.out[0, rows, c0 : c0 + value.shape[1]] = value.astype(BF16)


class Stream:
    def __init__(self, wire, first, partial, recv1, recv2, recv3, sends, sums, c0, far=False):
        self.first, self.partial, self.far = first, partial, far
        self.second = "y" if first == "x" else "x"
        self.sums, self.c0 = sums, c0
        self.recv1, self.recv2, self.recv3 = recv1, recv2, recv3
        self.send1, self.send2, self.send3 = sends
        self.sem1 = [wire.sem() for _ in range(2)]
        self.sem2 = [wire.sem() for _ in range(2)]
        self.sem3 = wire.sem()

    def chunk(self, way, c):
        if self.far:
            x, y = (c, slice(None)) if self.first == "x" else (slice(None), c)
            return (x, y, *self.share(way))
        return (c, way) if self.first == "x" else (slice(None), way, c)

    def share(self, way):
        rows, cols = self.recv1.shape[-2:]
        if self.recv3.shape[-2] == rows:
            return (slice(None), pl.ds(cols * way, cols))
        return (pl.ds(rows * way, rows), slice(None))

    def own(self, way, c, j):
        x, y = (c, j) if self.first == "x" else (j, c)
        if self.far:
            return self.recv3[(x, y, *self.share(way))]
        return self.partial[x, way, y]


def kernel(
    x_hbm,
    dy_hbm,
    ids_hbm,
    comb_hbm,
    wg_hbm,
    wu_hbm,
    wd_hbm,
    ig_out,
    cg_out,
    gg_out,
    ug_out,
    dg_out,
    wg,
    wu,
    wd,
    x,
    dy,
    xt,
    act,
    dact,
    hid,
    hg,
    hc,
    hct,
    gd,
    ud,
    weight_rows,
    weight_cols,
    cg_part,
    cg_rows,
    cg_in,
    rg,
    rc,
    rz,
    pd,
    pg,
    pz,
    rd1,
    rg1,
    rz1,
    rd2,
    rg2,
    rz2,
    rd3,
    rg3,
    rz3,
    rf1,
    rf2,
    rf3,
    rn1,
    rn2,
    rn3,
    ids_ref,
    comb_ref,
    local_sem,
    remote_sem,
):
    dp, ex = lax.axis_index("dp"), lax.axis_index("expert")
    ix, zh, iy = lax.div(dp, 8), lax.rem(lax.div(dp, 4), 2), lax.rem(dp, 4)
    zl, core = lax.div(ex, 2), lax.rem(ex, 2)

    def at(a, b, c):
        return {"dp": a * 8 + b * 4 + c, "expert": ex}

    x_next, x_prev = at(mod4(ix + 1), zh, iy), at(mod4(ix - 1), zh, iy)
    y_next, y_prev = at(ix, zh, mod4(iy + 1)), at(ix, zh, mod4(iy - 1))
    z_far = at(ix, 1 - zh, iy)
    mate = {"dp": dp, "expert": zl * 2 + 1 - core}
    z_near = {"dp": dp, "expert": (1 - zl) * 2 + core}
    z_diag = {"dp": dp, "expert": (1 - zl) * 2 + 1 - core}

    small = [
        pltpu.make_async_copy(ids_hbm, ids_ref, local_sem.at[5]),
        pltpu.make_async_copy(comb_hbm, comb_ref, local_sem.at[6]),
    ]
    loads = [
        pltpu.make_async_copy(x_hbm, x.at[pl.ds(0, T)], local_sem.at[0]),
        pltpu.make_async_copy(dy_hbm, dy.at[pl.ds(0, T)], local_sem.at[1]),
        pltpu.make_async_copy(wg_hbm.at[0], wg, local_sem.at[2]),
        pltpu.make_async_copy(wu_hbm.at[0], wu, local_sem.at[3]),
        pltpu.make_async_copy(wd_hbm.at[0], wd, local_sem.at[4]),
    ]
    barrier = pltpu.get_barrier_semaphore()
    peers = (x_next, x_prev, y_next, y_prev, z_far, mate, z_near, z_diag)
    for peer in peers:
        pl.semaphore_signal(barrier, inc=1, device_id=peer, device_id_type=MESH)
    for load in small + loads:
        load.start()
    for load in small:
        load.wait()
    expert = lax.broadcasted_iota(jnp.int32, (8, T), 0)
    dense = jnp.zeros((8, T), F32)
    for k in range(2):
        dense += jnp.where(ids_ref[k : k + 1, :] == expert, comb_ref[k : k + 1, :], 0.0)
    weight_rows[0] = dense
    pl.semaphore_wait(barrier, len(peers))

    wire = Wire(remote_sem, mate)

    def slot_rows(ref, slot):
        return ref.at[pl.ds(slot * T, T)]

    def x_block(slot, j):
        return x.at[pl.ds(slot * T + 64 * j, 64)]

    def dy_block(slot, j):
        return dy.at[pl.ds(slot * T, T), pl.ds(256 * j, 256)]

    x_near_send, x_near = wire.group(slot_rows(x, 0)), [wire.sem() for _ in range(2)]
    x_mate_send, x_mate = wire.group(slot_rows(x, 0)), wire.sem()
    x_pass_send, x_diag = wire.group(slot_rows(x, 2)), [wire.sem() for _ in range(2)]
    dy_near_send, dy_near = wire.group(slot_rows(dy, 0)), [wire.sem() for _ in range(8)]
    dy_mate_send, dy_mate = wire.group(slot_rows(dy, 0)), wire.sem()
    dy_pass_send, dy_diag = wire.group(slot_rows(dy, 2)), [wire.sem() for _ in range(8)]
    w_send, w_in = wire.group(weight_rows.at[pl.ds(1, 3)]), wire.sem()

    for j, to in ((1, mate), (2, z_near), (3, z_diag)):
        wire.put(weight_rows.at[0], weight_rows.at[j], to, w_send, w_in)

    loads[0].wait()
    for j in range(2):
        wire.put(x_block(0, j), x_block(2, j), z_near, x_near_send, x_near[j])
    wire.put(slot_rows(x, 0), slot_rows(x, 1), mate, x_mate_send, x_mate)
    loads[1].wait()
    for j in range(8):
        wire.put(dy_block(0, j), dy_block(2, j), z_near, dy_near_send, dy_near[j])
    wire.put(slot_rows(dy, 0), slot_rows(dy, 1), mate, dy_mate_send, dy_mate)

    def pass_x(j):
        wire.arrived(x_block(2, j), x_near[j])
        wire.put(x_block(2, j), x_block(3, j), mate, x_pass_send, x_diag[j])

    def pass_dy(j):
        wire.arrived(dy_block(2, j), dy_near[j])
        wire.put(dy_block(2, j), dy_block(3, j), mate, dy_pass_send, dy_diag[j])

    def column_weights(slot):
        row = weight_rows[slot, pl.ds(ex, 1), :]
        weight_cols[slot * T : slot * T + T, :] = jnp.transpose(jnp.broadcast_to(row, (T, T)))

    def spread(start):
        col = weight_cols[pl.ds(start, 16), :]
        return jnp.concatenate([col] * 6, axis=1)

    def turned(r0):
        def body(j, carry):
            cols = pl.ds(pl.multiple_of(j * 256, 256), 256)
            xt[cols, r0 : r0 + 256] = jnp.transpose(x[r0 : r0 + 256, cols])
            return carry

        lax.fori_loop(0, D // 256, body, 0)

    def gated(rows, start):
        gate, up = act[rows, :], dact[rows, :]
        s = jax.nn.sigmoid(gate)
        a = gate * s
        h = a * up
        act[rows, :] = a
        dact[rows, :] = up * s * (1.0 + gate * (1.0 - s))
        hid[rows, :] = h
        hc[rows, :] = (h * spread(start)).astype(BF16)

    def hidden_turned(r0):
        def turn(n, carry):
            cols = pl.ds(pl.multiple_of(n * 256, 256), 256)
            hct[cols, r0 : r0 + 256] = jnp.transpose(hc[:, cols])
            return carry

        lax.fori_loop(0, FF // 256, turn, 0)

    def forward():
        def matmul(n, carry):
            cols = pl.ds(pl.multiple_of(n * 256, 256), 256)
            act[:, cols] = nn(x[0:256, :], wg[:, cols])
            dact[:, cols] = nn(x[0:256, :], wu[:, cols])
            return carry

        lax.fori_loop(0, FF // 256, matmul, 0, unroll=True)

        def pointwise(i, carry):
            start = pl.multiple_of(i * 16, 16)
            gated(pl.ds(start, 16), start)
            return carry

        lax.fori_loop(0, 16, pointwise, 0)
        hidden_turned(0)

    def other_matmul(b):
        def matmul(n, carry):
            cols = pl.ds(pl.multiple_of(n * 256, 256), 256)
            starts = (2 * T + 64 * b, 3 * T + 64 * b)
            left = jnp.concatenate([x[r : r + 64, :] for r in starts], axis=0)
            for out, w in ((act, wg), (dact, wu)):
                r = nn(left, w[:, cols])
                out[64 * b : 64 * b + 64, cols] = r[0:64]
                out[T + 64 * b : T + 64 * b + 64, cols] = r[64:128]
            return carry

        lax.fori_loop(0, FF // 256, matmul, 0, unroll=True)

    def other_pointwise(b):
        def pointwise(i, carry):
            start = 64 * b + T * lax.div(i, 4) + 16 * lax.rem(i, 4)
            start = pl.multiple_of(start, 16)
            gated(pl.ds(start, 16), pl.multiple_of(256 + start, 16))
            return carry

        lax.fori_loop(0, 8, pointwise, 0)
        if b == 1:
            hidden_turned(256)

    def hidden_part(r0, first, j0, width):
        def matmul(n, carry):
            cols = pl.ds(pl.multiple_of(n * 256, 256), 256)
            r = nt(dy[r0 : r0 + 256, j0 : j0 + width], wd[cols, j0 : j0 + width])
            hg[:, cols] = r if first else hg[:, cols] + r
            return carry

        lax.fori_loop(0, FF // 256, matmul, 0, unroll=True)

    def backward(r0):
        def pointwise(i, carry):
            rows = pl.ds(pl.multiple_of(i * 16, 16), 16)
            full = pl.ds(pl.multiple_of(r0 + i * 16, 16), 16)
            g = hg[rows, :]
            prod = g * hid[rows, :]
            total = prod[:, 0:128]
            for j in range(1, 6):
                total += prod[:, 128 * j : 128 * j + 128]
            cg_part[full, :] = total
            g = g * spread(pl.multiple_of(r0 + i * 16, 16))
            gd[full, :] = (g * dact[rows, :]).astype(BF16)
            ud[full, :] = (g * act[rows, :]).astype(BF16)
            return carry

        lax.fori_loop(0, 16, pointwise, 0)

    loads[2].wait()
    loads[3].wait()
    wire.arrived(slot_rows(x, 1), x_mate)
    wire.arrived(weight_rows.at[pl.ds(1, 3)], w_in)
    for slot in range(4):
        column_weights(slot)
    forward()
    pass_x(0)
    turned(0)
    loads[4].wait()
    wire.arrived(slot_rows(dy, 1), dy_mate)
    hidden_part(0, True, 0, D)
    backward(0)
    wire.arrived(x_block(3, 0), x_diag[0])
    other_matmul(0)
    pass_x(1)
    other_pointwise(0)
    pass_dy(0)
    wire.arrived(x_block(3, 1), x_diag[1])

    down = Sums(None, dg_out)
    gate = Sums(gd, gg_out)
    upper = Sums(ud, ug_out)
    d_sends = [wire.group(ref) for ref in (rd1, rd2, rd3)]
    g_sends = [wire.group(ref) for ref in (rg1, rg2, rg3)]
    z_sends = [wire.group(ref) for ref in (rz1, rz2, rz3)]
    def axis(j):
        return "xy"[j % 2]

    d = [
        Stream(wire, axis(j), pd.at[j], rd1.at[j], rd2.at[j], rd3.at[j], d_sends, down, 256 * j)
        for j in range(7)
    ]
    far_sends = [wire.group(ref) for ref in (rf1, rf2, rf3)]
    far_down = Stream(wire, "x", pd.at[7], rf1, rf2, rf3, far_sends, down, 1792, True)
    narrow_sends = [wire.group(ref) for ref in (rn1, rn2, rn3)]
    narrow = Stream(wire, "y", pz.at[3], rn1, rn2, rn3, narrow_sends, upper, 640)
    up = [
        Stream(wire, axis(j), pg.at[j], rg1.at[j], rg2.at[j], rg3.at[j], g_sends, sums, 256 * (j % 2))
        for j, sums in enumerate((gate, gate, upper, upper))
    ]
    far = [
        Stream(wire, axis(j), pz.at[j], rz1.at[j], rz2.at[j], rz3.at[j], z_sends, sums, c0, True)
        for j, (sums, c0) in enumerate(((gate, 512), (gate, 640), (upper, 512)))
    ]

    def ring(first, way):
        i = ix if first == "x" else iy
        near = (x_next, x_prev) if first == "x" else (y_next, y_prev)
        return i, 1 - 2 * way, near[way], near[1 - way]

    def launch_relay(st):
        source = st.recv3 if st.far else st.partial
        for way in range(2):
            i, sign, ahead, behind = ring(st.first, way)
            src = source.at[st.chunk(way, mod4(i + 2))]
            wire.put(src, st.recv1.at[way, 0], behind, st.send1, st.sem1[0])

    def launch_direct(st):
        source = st.recv3 if st.far else st.partial
        for way in range(2):
            i, sign, ahead, behind = ring(st.first, way)
            src = source.at[st.chunk(way, mod4(i + sign))]
            wire.put(src, st.recv1.at[way, 1], ahead, st.send1, st.sem1[1])

    def launch(st):
        launch_relay(st)
        launch_direct(st)

    def down_part(j):
        wire.arrived(dy_block(3, j), dy_diag[j])
        r = nn(hct[...], dy[:, 256 * j : 256 * j + 256]).reshape(4, 2, 4, 24, 256)
        pd[j] = r.astype(BF16)
        if j < 7:
            launch(d[j])
        else:
            wire.put(pd.at[7, :, 1 - zh], rf3, z_far, far_down.send3, far_down.sem3)

    def up_chunk(st, away):
        right, c0 = st.sums.right, st.c0
        for way in range(2):
            i, sign, ahead, behind = ring(st.first, way)
            c = mod4(i + away * sign)
            if st.first == "x":
                rows = pl.multiple_of(c * 512 + way * 256, 256)
                left = xt[pl.ds(rows, 256), :]
            else:
                starts = [pl.multiple_of(j * 512 + way * 256 + c * 64, 64) for j in range(4)]
                left = jnp.concatenate([xt[pl.ds(r, 64), :] for r in starts], axis=0)
            r = nn(left, right[:, c0 : c0 + 256]).astype(BF16).reshape(4, 64, 256)
            if st.first == "x":
                st.partial[c, way] = r
            else:
                for j in range(4):
                    st.partial[j, way, c] = r[j]

    def up_first(st):
        up_chunk(st, 2)
        launch_relay(st)

    def up_rest(st):
        up_chunk(st, 1)
        launch_direct(st)

        up_chunk(st, -1)
        up_chunk(st, 0)

    def far_part(kind, half):
        right, k = (gd, ud)[kind], 2 * kind

        def body(c, carry):
            rows = pl.multiple_of(c * 512 + half * 256, 256)
            r = nn(xt[pl.ds(rows, 256), :], right[:, 512:768]).astype(BF16)
            r = r.reshape(4, 64, 256)
            pz[k, c, half] = r[:, :, 0:128]
            pz[k + 1, c, half] = r[:, :, 128:256]
            return carry

        lax.fori_loop(0, 4, body, 0, unroll=True)

    def far_first(kind):
        far_part(kind, 1 - zh)
        for st in far[2 * kind : 2 * kind + 2]:
            wire.put(st.partial.at[:, 1 - zh], st.recv3, z_far, st.send3, st.sem3)

    def far_sum(st):
        wire.arrived(st.recv3, st.sem3)

        def body(c, carry):
            for j in range(4):
                total = st.recv3[c, j].astype(F32) + st.partial[c, zh, j].astype(F32)
                st.recv3[c, j] = total.astype(BF16)
            return carry

        lax.fori_loop(0, 4, body, 0)
        launch(st)

    def step1(st, s):
        if s == 0:
            wire.arrived(st.recv1.at[:, 0], st.sem1[0])
        else:
            wire.arrived(st.recv1.at[:, pl.ds(1, 2)], st.sem1[1])
        for way in range(2):
            i, sign, ahead, behind = ring(st.first, way)
            c = mod4(i - sign) if s == 0 else i
            for j in range(4):
                total = st.recv1[way, s, j].astype(F32) + st.own(way, c, j).astype(F32)
                if s == 1:
                    total += st.recv1[way, 2, j].astype(F32)
                st.recv1[way, 2 * s, j] = total.astype(BF16)
            if s == 0:
                wire.put(st.recv1.at[way, 0], st.recv1.at[way, 2], behind, st.send1, st.sem1[1])
        if s == 1:
            for way in range(2):
                i, sign, ahead, behind = ring(st.second, way)
                src = st.recv1.at[way, 2, mod4(i + 2)]
                wire.put(src, st.recv2.at[way, 0], behind, st.send2, st.sem2[0])
            for way in range(2):
                i, sign, ahead, behind = ring(st.second, way)
                src = st.recv1.at[way, 2, mod4(i + sign)]
                wire.put(src, st.recv2.at[way, 1], ahead, st.send2, st.sem2[1])

    def step2(st, s):
        if s == 0:
            wire.arrived(st.recv2.at[:, 0], st.sem2[0])
        else:
            wire.arrived(st.recv2.at[:, pl.ds(1, 2)], st.sem2[1])
        for way in range(2):
            i, sign, ahead, behind = ring(st.second, way)
            c = mod4(i - sign) if s == 0 else i
            total = st.recv2[way, s].astype(F32) + st.recv1[way, 2, c].astype(F32)
            if s == 0:
                st.recv2[way, 0] = total.astype(BF16)
                wire.put(st.recv2.at[way, 0], st.recv2.at[way, 2], behind, st.send2, st.sem2[1])
                continue
            total += st.recv2[way, 2].astype(F32)
            if st.far:
                rows, cols = total.shape
                if st.recv3.shape[-2] == rows:
                    st.sums.put(slice(None), st.c0 + cols * way, total)
                else:
                    st.sums.put(slice(rows * way, rows * way + rows), st.c0, total)
            else:
                st.recv2[way, 2] = total.astype(BF16)
        if s == 1 and not st.far:
            wire.put(st.recv2.at[1 - zh, 2], st.recv3, z_far, st.send3, st.sem3)

    def result(st):
        wire.arrived(st.recv3, st.sem3)
        total = st.recv2[zh, 2].astype(F32) + st.recv3[...].astype(F32)
        st.sums.put(slice(None), st.c0, total)

    rc_send, rc_far, rc_near = wire.group(rc), wire.sem(), wire.sem()
    rz_send, rz_in = wire.group(rz), wire.sem()
    cg_send, cg_sem = wire.group(cg_rows.at[pl.ds(1, 3)]), wire.sem()

    def row_part(half, q):
        r0 = 256 * half

        def body(n, carry):
            cols = pl.ds(pl.multiple_of(q * 512 + n * 256, 256), 256)
            r = nt(gd[r0 : r0 + 256, :], wg[cols, :]) + nt(ud[r0 : r0 + 256, :], wu[cols, :])
            rg[r0 : r0 + 256, cols] = r.astype(BF16)
            return carry

        lax.fori_loop(0, 2, body, 0, unroll=True)
        if q == 3:
            if half == 1:
                wire.put(slot_rows(rg, 3), rc.at[1], mate, rc_send, rc_far)
            else:
                wire.put(slot_rows(rg, 1), rc.at[0], mate, rc_send, rc_near)

    def add_far():
        wire.arrived(rc.at[1], rc_far)

        def body(i, carry):
            rows = pl.ds(pl.multiple_of(i * 16, 16), 16)
            full = pl.ds(pl.multiple_of(2 * T + i * 16, 16), 16)
            total = rg[full, :].astype(F32) + rc[1, rows, :].astype(F32)
            rg[full, :] = total.astype(BF16)
            return carry

        lax.fori_loop(0, T // 16, body, 0)
        wire.put(slot_rows(rg, 2), rz, z_near, rz_send, rz_in)

    def add_rows():
        wire.arrived(rc.at[0], rc_near)
        wire.arrived(rz, rz_in)

        def body(i, carry):
            rows = pl.ds(pl.multiple_of(i * 16, 16), 16)
            total = rg[rows, :].astype(F32) + rc[0, rows, :].astype(F32)
            ig_out[rows, :] = (total + rz[rows, :].astype(F32)).astype(BF16)
            return carry

        lax.fori_loop(0, T // 16, body, 0)

    def combine_part():
        for slot in range(4):
            part = jnp.transpose(cg_part[slot * T : slot * T + T, :])
            cg_rows[slot] = jnp.broadcast_to(jnp.sum(part, axis=0, keepdims=True), (8, T))
        for j, to in ((1, mate), (2, z_near), (3, z_diag)):
            wire.put(cg_rows.at[j], cg_in.at[j], to, cg_send, cg_sem)

    def combine_result():
        wire.arrived(cg_in.at[pl.ds(1, 3)], cg_sem)
        answer = jnp.zeros((2, T), F32)
        for j in range(4):
            row = cg_rows[0, 0:1, :] if j == 0 else cg_in[j, 0:1, :]
            answer += jnp.where(ids_ref[...] == jnp.bitwise_xor(ex, j), row, 0.0)
        cg_out[...] = answer

    other_matmul(1)
    pass_dy(1)
    other_pointwise(1)
    down_part(0)
    pass_dy(2)
    turned(256)
    pass_dy(3)
    down_part(1)
    down_part(2)
    pass_dy(4)
    down_part(3)
    pass_dy(5)
    hidden_part(256, True, 0, 512)
    step1(d[0], 0)
    hidden_part(256, False, 512, 512)
    pass_dy(6)
    down_part(4)
    step1(d[1], 0)
    down_part(5)
    pass_dy(7)
    hidden_part(256, False, 1024, 512)
    step1(d[2], 0)
    down_part(6)
    step1(d[3], 0)
    down_part(7)
    step1(d[0], 1)
    hidden_part(256, False, 1536, 512)
    backward(256)
    step1(d[4], 0)
    up_first(up[0])
    far_first(0)
    step1(d[5], 0)
    far_first(1)
    up_first(up[1])
    up_first(up[2])
    up_first(up[3])
    step1(d[1], 1)
    step1(d[2], 1)
    far_part(0, zh)
    far_part(1, zh)
    launch_relay(narrow)
    step2(d[0], 0)
    launch_direct(narrow)
    up_rest(up[1])
    step1(d[4], 1)
    up_rest(up[3])
    step1(d[6], 0)
    up_rest(up[2])
    far_sum(far_down)
    step1(d[3], 1)
    combine_part()
    row_part(1, 0)
    step1(up[1], 0)
    row_part(1, 1)
    row_part(1, 2)
    step1(up[2], 0)
    step2(d[1], 0)
    step1(up[3], 0)
    step1(d[6], 1)
    far_sum(far[0])
    up_rest(up[0])
    step1(up[0], 0)
    step1(narrow, 0)
    step2(d[0], 1)
    step1(d[5], 1)
    step2(d[2], 0)
    step1(far_down, 0)
    row_part(1, 3)
    step2(d[4], 0)
    row_part(0, 0)
    row_part(0, 1)
    far_sum(far[1])
    step1(up[2], 1)
    row_part(0, 2)
    step2(d[1], 1)
    row_part(0, 3)
    add_far()
    step1(far[0], 0)
    step2(d[3], 0)
    far_sum(far[2])
    step1(up[3], 1)
    step1(up[0], 1)
    step2(d[5], 0)
    step2(d[6], 0)
    step1(far_down, 1)
    step1(up[1], 1)
    result(d[1])
    step1(narrow, 1)
    step1(far[0], 1)
    step2(d[2], 1)
    step2(d[3], 1)
    step1(far[2], 0)
    step1(far[1], 0)
    step2(up[3], 0)
    step2(up[2], 0)
    step2(d[5], 1)
    step2(up[0], 0)
    step2(up[1], 0)
    step2(d[4], 1)
    step2(d[6], 1)
    step2(narrow, 0)
    step2(far[0], 0)
    step1(far[2], 1)
    step1(far[1], 1)
    step2(up[3], 1)
    step2(up[2], 1)
    step2(far_down, 0)
    step2(up[0], 1)
    add_rows()
    step2(up[1], 1)
    result(d[2])
    combine_result()
    result(d[3])
    result(d[5])
    step2(narrow, 1)
    step2(far[0], 1)
    result(d[4])
    result(d[6])
    step2(far[2], 0)
    step2(far[1], 0)
    result(d[0])
    result(up[3])
    step2(far_down, 1)
    result(up[0])
    step2(far[2], 1)
    step2(far[1], 1)
    result(up[1])
    result(up[2])
    result(narrow)

    wire.finish()


def hand_over(*refs):
    for src, dst in zip(refs[:5], refs[5:]):
        dst[...] = src[...]


OUTS = (
    jax.ShapeDtypeStruct((T, D), BF16),
    jax.ShapeDtypeStruct((2, T), F32),
    jax.ShapeDtypeStruct((1, 64, FF), BF16),
    jax.ShapeDtypeStruct((1, 64, FF), BF16),
    jax.ShapeDtypeStruct((1, 24, D), BF16),
)


def shards(tokens, cotangent, expert_ids, combine, w_gate, w_up, w_down):
    hbm = pl.BlockSpec(memory_space=pl.ANY)
    vmem = pl.BlockSpec(memory_space=pltpu.VMEM)
    outs = pl.pallas_call(
        kernel,
        out_shape=tuple(pltpu.VMEM(o.shape, o.dtype) for o in OUTS),
        in_specs=[hbm] * 7,
        out_specs=(vmem,) * 5,
        scratch_shapes=[
            pltpu.VMEM((D, FF), BF16),
            pltpu.VMEM((D, FF), BF16),
            pltpu.VMEM((FF, D), BF16),
            pltpu.VMEM((4 * T, D), BF16),
            pltpu.VMEM((4 * T, D), BF16),
            pltpu.VMEM((D, 4 * T), BF16),
            pltpu.VMEM((256, FF), F32),
            pltpu.VMEM((256, FF), F32),
            pltpu.VMEM((256, FF), F32),
            pltpu.VMEM((256, FF), F32),
            pltpu.VMEM((256, FF), BF16),
            pltpu.VMEM((FF, 4 * T), BF16),
            pltpu.VMEM((4 * T, FF), BF16),
            pltpu.VMEM((4 * T, FF), BF16),
            pltpu.VMEM((4, 8, T), F32),
            pltpu.VMEM((4 * T, T), F32),
            pltpu.VMEM((4 * T, T), F32),
            pltpu.VMEM((4, 8, T), F32),
            pltpu.VMEM((4, 8, T), F32),
            pltpu.VMEM((4 * T, D), BF16),
            pltpu.VMEM((2, T, D), BF16),
            pltpu.VMEM((T, D), BF16),
            pltpu.VMEM((8, 4, 2, 4, 24, 256), BF16),
            pltpu.VMEM((4, 4, 2, 4, 64, 256), BF16),
            pltpu.VMEM((4, 4, 2, 4, 64, 128), BF16),
            pltpu.VMEM((7, 2, 3, 4, 24, 256), BF16),
            pltpu.VMEM((4, 2, 3, 4, 64, 256), BF16),
            pltpu.VMEM((3, 2, 3, 4, 32, 128), BF16),
            pltpu.VMEM((7, 2, 3, 24, 256), BF16),
            pltpu.VMEM((4, 2, 3, 64, 256), BF16),
            pltpu.VMEM((3, 2, 3, 32, 128), BF16),
            pltpu.VMEM((7, 24, 256), BF16),
            pltpu.VMEM((4, 64, 256), BF16),
            pltpu.VMEM((3, 4, 4, 64, 128), BF16),
            pltpu.VMEM((2, 3, 4, 24, 128), BF16),
            pltpu.VMEM((2, 3, 24, 128), BF16),
            pltpu.VMEM((4, 4, 24, 256), BF16),
            pltpu.VMEM((2, 3, 4, 64, 128), BF16),
            pltpu.VMEM((2, 3, 64, 128), BF16),
            pltpu.VMEM((64, 128), BF16),
            pltpu.VMEM((2, T), jnp.int32),
            pltpu.VMEM((2, T), F32),
            pltpu.SemaphoreType.DMA((7,)),
            pltpu.SemaphoreType.DMA((N_SEM,)),
        ],
        compiler_params=pltpu.CompilerParams(
            collective_id=0, has_side_effects=True, vmem_limit_bytes=60 * 1024 * 1024
        ),
        name="experts",
    )(tokens, cotangent, expert_ids.T, combine.T, w_gate, w_up, w_down)
    outs = pl.pallas_call(
        hand_over,
        out_shape=OUTS,
        in_specs=[vmem] * 5,
        out_specs=(vmem,) * 5,
        name="hand_over",
    )(*(pltpu.with_memory_space_constraint(o, pltpu.VMEM) for o in outs))
    return (outs[0], outs[1].T, *outs[2:])


def solution(mesh):
    both = ("dp", "expert")
    return jax.shard_map(
        shards,
        mesh=mesh,
        in_specs=(
            P(both, None),
            P(both, None),
            P(both, None),
            P(both, None),
            P("expert", None, None),
            P("expert", None, None),
            P("expert", None, None),
        ),
        out_specs=(
            P(both, None),
            P(both, None),
            P("expert", "dp", None),
            P("expert", "dp", None),
            P("expert", "dp", None),
        ),
        check_vma=False,
    )
```

```python
import jax
import jax.numpy as jnp
from jax import lax
from jax.experimental import pallas as pl
from jax.experimental.pallas import tpu as pltpu
from jax.sharding import PartitionSpec as P

MESH = pl.DeviceIdType.MESH
BF16 = jnp.bfloat16
F32 = jnp.float32
D = 2048
FF = 768
T = 128
N_SEM = 132


def mod4(v):
    return lax.rem(v + 8, 4)


def nt(a, b):
    return lax.dot_general(a, b, (((1,), (1,)), ((), ())), preferred_element_type=F32)


def nn(a, b):
    return jnp.dot(a, b, preferred_element_type=F32)


class Wire:
    def __init__(self, sems, other):
        self.sems, self.other, self.count, self.groups = sems, other, 0, []

    def sem(self):
        self.count += 1
        return self.sems.at[self.count - 1]

    def describe(self, src, dst, send, recv, device):
        return pltpu.make_async_remote_copy(
            src_ref=src,
            dst_ref=dst,
            send_sem=send,
            recv_sem=recv,
            device_id=device,
            device_id_type=MESH,
        )

    def group(self, total):
        send = self.sem()
        self.groups.append((send, total))
        return send

    def put(self, src, dst, device, send, recv):
        self.describe(src, dst, send, recv, device).start()

    def arrived(self, ref, recv):
        self.describe(ref, ref, recv, recv, self.other).wait_recv()

    def finish(self):
        for send, total in self.groups:
            self.describe(total, total, send, send, self.other).wait_send()


class Sums:
    def __init__(self, right, out):
        self.right, self.out = right, out

    def put(self, rows, c0, value):
        self.out[0, rows, c0 : c0 + value.shape[1]] = value.astype(BF16)


class Stream:
    def __init__(self, wire, first, partial, recv1, recv2, recv3, sends, sums, c0, far=False):
        self.first, self.partial, self.far = first, partial, far
        self.second = "y" if first == "x" else "x"
        self.sums, self.c0 = sums, c0
        self.recv1, self.recv2, self.recv3 = recv1, recv2, recv3
        self.send1, self.send2, self.send3 = sends
        self.sem1 = [wire.sem() for _ in range(2)]
        self.sem2 = [wire.sem() for _ in range(2)]
        self.sem3 = wire.sem()

    def chunk(self, way, c):
        if self.far:
            x, y = (c, slice(None)) if self.first == "x" else (slice(None), c)
            return (x, y, *self.share(way))
        return (c, way) if self.first == "x" else (slice(None), way, c)

    def share(self, way):
        rows, cols = self.recv1.shape[-2:]
        if self.recv3.shape[-2] == rows:
            return (slice(None), pl.ds(cols * way, cols))
        return (pl.ds(rows * way, rows), slice(None))

    def own(self, way, c, j):
        x, y = (c, j) if self.first == "x" else (j, c)
        if self.far:
            return self.recv3[(x, y, *self.share(way))]
        return self.partial[x, way, y]


def kernel(
    x_hbm,
    dy_hbm,
    ids_hbm,
    comb_hbm,
    wg_hbm,
    wu_hbm,
    wd_hbm,
    ig_out,
    cg_out,
    gg_out,
    ug_out,
    dg_out,
    wg,
    wu,
    wd,
    x,
    dy,
    xt,
    act,
    dact,
    hid,
    hg,
    hc,
    hct,
    gd,
    ud,
    weight_rows,
    weight_cols,
    cg_part,
    cg_rows,
    cg_in,
    rg,
    rc,
    rz,
    pd,
    pg,
    pz,
    rd1,
    rg1,
    rz1,
    rd2,
    rg2,
    rz2,
    rd3,
    rg3,
    rz3,
    rf1,
    rf2,
    rf3,
    rn1,
    rn2,
    rn3,
    ids_ref,
    comb_ref,
    local_sem,
    remote_sem,
):
    dp, ex = lax.axis_index("dp"), lax.axis_index("expert")
    ix, zh, iy = lax.div(dp, 8), lax.rem(lax.div(dp, 4), 2), lax.rem(dp, 4)
    zl, core = lax.div(ex, 2), lax.rem(ex, 2)

    def at(a, b, c):
        return {"dp": a * 8 + b * 4 + c, "expert": ex}

    x_next, x_prev = at(mod4(ix + 1), zh, iy), at(mod4(ix - 1), zh, iy)
    y_next, y_prev = at(ix, zh, mod4(iy + 1)), at(ix, zh, mod4(iy - 1))
    z_far = at(ix, 1 - zh, iy)
    mate = {"dp": dp, "expert": zl * 2 + 1 - core}
    z_near = {"dp": dp, "expert": (1 - zl) * 2 + core}
    z_diag = {"dp": dp, "expert": (1 - zl) * 2 + 1 - core}

    small = [
        pltpu.make_async_copy(ids_hbm, ids_ref, local_sem.at[5]),
        pltpu.make_async_copy(comb_hbm, comb_ref, local_sem.at[6]),
    ]
    loads = [
        pltpu.make_async_copy(x_hbm, x.at[pl.ds(0, T)], local_sem.at[0]),
        pltpu.make_async_copy(dy_hbm, dy.at[pl.ds(0, T)], local_sem.at[1]),
        pltpu.make_async_copy(wg_hbm.at[0], wg, local_sem.at[2]),
        pltpu.make_async_copy(wu_hbm.at[0], wu, local_sem.at[3]),
        pltpu.make_async_copy(wd_hbm.at[0], wd, local_sem.at[4]),
    ]
    barrier = pltpu.get_barrier_semaphore()
    peers = (x_next, x_prev, y_next, y_prev, z_far, mate, z_near, z_diag)
    for peer in peers:
        pl.semaphore_signal(barrier, inc=1, device_id=peer, device_id_type=MESH)
    for load in loads[0:1] + small + loads[1:2]:
        load.start()
    for load in small:
        load.wait()
    expert = lax.broadcasted_iota(jnp.int32, (8, T), 0)
    dense = jnp.zeros((8, T), F32)
    for k in range(2):
        dense += jnp.where(ids_ref[k : k + 1, :] == expert, comb_ref[k : k + 1, :], 0.0)
    weight_rows[0] = dense
    pl.semaphore_wait(barrier, len(peers))

    wire = Wire(remote_sem, mate)

    def slot_rows(ref, slot):
        return ref.at[pl.ds(slot * T, T)]

    def x_block(slot, j):
        return x.at[pl.ds(slot * T + 64 * j, 64)]

    def dy_block(slot, j):
        return dy.at[pl.ds(slot * T, T), pl.ds(256 * j, 256)]

    x_near_send, x_near = wire.group(slot_rows(x, 0)), [wire.sem() for _ in range(2)]
    x_mate_send, x_mate = wire.group(slot_rows(x, 0)), wire.sem()
    x_pass_send, x_diag = wire.group(slot_rows(x, 2)), [wire.sem() for _ in range(2)]
    dy_near_send, dy_near = wire.group(slot_rows(dy, 0)), [wire.sem() for _ in range(8)]
    dy_mate_send, dy_mate = wire.group(slot_rows(dy, 0)), wire.sem()
    dy_pass_send, dy_diag = wire.group(slot_rows(dy, 2)), [wire.sem() for _ in range(8)]
    w_send, w_in = wire.group(weight_rows.at[pl.ds(1, 3)]), wire.sem()

    loads[0].wait()
    for j, to in ((1, mate), (2, z_near), (3, z_diag)):
        wire.put(weight_rows.at[0], weight_rows.at[j], to, w_send, w_in)
    for j in range(2):
        wire.put(x_block(0, j), x_block(2, j), z_near, x_near_send, x_near[j])
    wire.put(slot_rows(x, 0), slot_rows(x, 1), mate, x_mate_send, x_mate)
    for load in loads[2:5]:
        load.start()
    loads[1].wait()
    for j in range(8):
        wire.put(dy_block(0, j), dy_block(2, j), z_near, dy_near_send, dy_near[j])
    wire.put(slot_rows(dy, 0), slot_rows(dy, 1), mate, dy_mate_send, dy_mate)

    def pass_x(j):
        wire.arrived(x_block(2, j), x_near[j])
        wire.put(x_block(2, j), x_block(3, j), mate, x_pass_send, x_diag[j])

    def pass_dy(j):
        wire.arrived(dy_block(2, j), dy_near[j])
        wire.put(dy_block(2, j), dy_block(3, j), mate, dy_pass_send, dy_diag[j])

    def column_weights(slot):
        row = weight_rows[slot, pl.ds(ex, 1), :]
        weight_cols[slot * T : slot * T + T, :] = jnp.transpose(jnp.broadcast_to(row, (T, T)))

    def spread(start):
        col = weight_cols[pl.ds(start, 16), :]
        return jnp.concatenate([col] * 6, axis=1)

    def turned(r0):
        def body(j, carry):
            cols = pl.ds(pl.multiple_of(j * 256, 256), 256)
            xt[cols, r0 : r0 + 256] = jnp.transpose(x[r0 : r0 + 256, cols])
            return carry

        lax.fori_loop(0, D // 256, body, 0)

    def gated(rows, start):
        gate, up = act[rows, :], dact[rows, :]
        s = jax.nn.sigmoid(gate)
        a = gate * s
        h = a * up
        act[rows, :] = a
        dact[rows, :] = up * s * (1.0 + gate * (1.0 - s))
        hid[rows, :] = h
        hc[rows, :] = (h * spread(start)).astype(BF16)

    def hidden_turned(r0):
        def turn(n, carry):
            cols = pl.ds(pl.multiple_of(n * 256, 256), 256)
            hct[cols, r0 : r0 + 256] = jnp.transpose(hc[:, cols])
            return carry

        lax.fori_loop(0, FF // 256, turn, 0)

    def forward():
        def matmul(n, carry):
            cols = pl.ds(pl.multiple_of(n * 256, 256), 256)
            act[:, cols] = nn(x[0:256, :], wg[:, cols])
            dact[:, cols] = nn(x[0:256, :], wu[:, cols])
            return carry

        lax.fori_loop(0, FF // 256, matmul, 0, unroll=True)

        def pointwise(i, carry):
            start = pl.multiple_of(i * 16, 16)
            gated(pl.ds(start, 16), start)
            return carry

        lax.fori_loop(0, 16, pointwise, 0)
        hidden_turned(0)

    def other_matmul(b):
        def matmul(n, carry):
            cols = pl.ds(pl.multiple_of(n * 256, 256), 256)
            starts = (2 * T + 64 * b, 3 * T + 64 * b)
            left = jnp.concatenate([x[r : r + 64, :] for r in starts], axis=0)
            for out, w in ((act, wg), (dact, wu)):
                r = nn(left, w[:, cols])
                out[64 * b : 64 * b + 64, cols] = r[0:64]
                out[T + 64 * b : T + 64 * b + 64, cols] = r[64:128]
            return carry

        lax.fori_loop(0, FF // 256, matmul, 0, unroll=True)

    def other_pointwise(b):
        def pointwise(i, carry):
            start = 64 * b + T * lax.div(i, 4) + 16 * lax.rem(i, 4)
            start = pl.multiple_of(start, 16)
            gated(pl.ds(start, 16), pl.multiple_of(256 + start, 16))
            return carry

        lax.fori_loop(0, 8, pointwise, 0)
        if b == 1:
            hidden_turned(256)

    def hidden_part(r0, first, j0, width):
        def matmul(n, carry):
            cols = pl.ds(pl.multiple_of(n * 256, 256), 256)
            r = nt(dy[r0 : r0 + 256, j0 : j0 + width], wd[cols, j0 : j0 + width])
            hg[:, cols] = r if first else hg[:, cols] + r
            return carry

        lax.fori_loop(0, FF // 256, matmul, 0, unroll=True)

    def backward(r0):
        def pointwise(i, carry):
            rows = pl.ds(pl.multiple_of(i * 16, 16), 16)
            full = pl.ds(pl.multiple_of(r0 + i * 16, 16), 16)
            g = hg[rows, :]
            prod = g * hid[rows, :]
            total = prod[:, 0:128]
            for j in range(1, 6):
                total += prod[:, 128 * j : 128 * j + 128]
            cg_part[full, :] = total
            g = g * spread(pl.multiple_of(r0 + i * 16, 16))
            gd[full, :] = (g * dact[rows, :]).astype(BF16)
            ud[full, :] = (g * act[rows, :]).astype(BF16)
            return carry

        lax.fori_loop(0, 16, pointwise, 0)

    loads[2].wait()
    loads[3].wait()
    wire.arrived(slot_rows(x, 1), x_mate)
    wire.arrived(weight_rows.at[pl.ds(1, 3)], w_in)
    for slot in range(4):
        column_weights(slot)
    forward()
    pass_x(0)
    turned(0)
    loads[4].wait()
    wire.arrived(slot_rows(dy, 1), dy_mate)
    hidden_part(0, True, 0, D)
    backward(0)
    wire.arrived(x_block(3, 0), x_diag[0])
    other_matmul(0)
    pass_x(1)
    other_pointwise(0)
    pass_dy(0)
    wire.arrived(x_block(3, 1), x_diag[1])

    down = Sums(None, dg_out)
    gate = Sums(gd, gg_out)
    upper = Sums(ud, ug_out)
    d_sends = [wire.group(ref) for ref in (rd1, rd2, rd3)]
    g_sends = [wire.group(ref) for ref in (rg1, rg2, rg3)]
    z_sends = [wire.group(ref) for ref in (rz1, rz2, rz3)]
    def axis(j):
        return "xy"[j % 2]

    d = [
        Stream(wire, axis(j), pd.at[j], rd1.at[j], rd2.at[j], rd3.at[j], d_sends, down, 256 * j)
        for j in range(7)
    ]
    far_sends = [wire.group(ref) for ref in (rf1, rf2, rf3)]
    far_down = Stream(wire, "x", pd.at[7], rf1, rf2, rf3, far_sends, down, 1792, True)
    narrow_sends = [wire.group(ref) for ref in (rn1, rn2, rn3)]
    narrow = Stream(wire, "y", pz.at[3], rn1, rn2, rn3, narrow_sends, upper, 640)
    up = [
        Stream(wire, axis(j), pg.at[j], rg1.at[j], rg2.at[j], rg3.at[j], g_sends, sums, 256 * (j % 2))
        for j, sums in enumerate((gate, gate, upper, upper))
    ]
    far = [
        Stream(wire, axis(j), pz.at[j], rz1.at[j], rz2.at[j], rz3.at[j], z_sends, sums, c0, True)
        for j, (sums, c0) in enumerate(((gate, 512), (gate, 640), (upper, 512)))
    ]

    def ring(first, way):
        i = ix if first == "x" else iy
        near = (x_next, x_prev) if first == "x" else (y_next, y_prev)
        return i, 1 - 2 * way, near[way], near[1 - way]

    def launch_relay(st):
        source = st.recv3 if st.far else st.partial
        for way in range(2):
            i, sign, ahead, behind = ring(st.first, way)
            src = source.at[st.chunk(way, mod4(i + 2))]
            wire.put(src, st.recv1.at[way, 0], behind, st.send1, st.sem1[0])

    def launch_direct(st):
        source = st.recv3 if st.far else st.partial
        for way in range(2):
            i, sign, ahead, behind = ring(st.first, way)
            src = source.at[st.chunk(way, mod4(i + sign))]
            wire.put(src, st.recv1.at[way, 1], ahead, st.send1, st.sem1[1])

    def launch(st):
        launch_relay(st)
        launch_direct(st)

    def down_part(j):
        wire.arrived(dy_block(3, j), dy_diag[j])
        r = nn(hct[...], dy[:, 256 * j : 256 * j + 256]).reshape(4, 2, 4, 24, 256)
        pd[j] = r.astype(BF16)
        if j < 7:
            launch(d[j])
        else:
            wire.put(pd.at[7, :, 1 - zh], rf3, z_far, far_down.send3, far_down.sem3)

    def up_chunk(st, away):
        right, c0 = st.sums.right, st.c0
        for way in range(2):
            i, sign, ahead, behind = ring(st.first, way)
            c = mod4(i + away * sign)
            if st.first == "x":
                rows = pl.multiple_of(c * 512 + way * 256, 256)
                left = xt[pl.ds(rows, 256), :]
            else:
                starts = [pl.multiple_of(j * 512 + way * 256 + c * 64, 64) for j in range(4)]
                left = jnp.concatenate([xt[pl.ds(r, 64), :] for r in starts], axis=0)
            r = nn(left, right[:, c0 : c0 + 256]).astype(BF16).reshape(4, 64, 256)
            if st.first == "x":
                st.partial[c, way] = r
            else:
                for j in range(4):
                    st.partial[j, way, c] = r[j]

    def up_first(st):
        up_chunk(st, 2)
        launch_relay(st)

    def up_rest(st):
        up_chunk(st, 1)
        launch_direct(st)

        up_chunk(st, -1)
        up_chunk(st, 0)

    def far_part(kind, half):
        right, k = (gd, ud)[kind], 2 * kind

        def body(c, carry):
            rows = pl.multiple_of(c * 512 + half * 256, 256)
            r = nn(xt[pl.ds(rows, 256), :], right[:, 512:768]).astype(BF16)
            r = r.reshape(4, 64, 256)
            pz[k, c, half] = r[:, :, 0:128]
            pz[k + 1, c, half] = r[:, :, 128:256]
            return carry

        lax.fori_loop(0, 4, body, 0, unroll=True)

    def far_first(kind):
        far_part(kind, 1 - zh)
        for st in far[2 * kind : 2 * kind + 2]:
            wire.put(st.partial.at[:, 1 - zh], st.recv3, z_far, st.send3, st.sem3)

    def far_sum(st):
        wire.arrived(st.recv3, st.sem3)

        def body(c, carry):
            for j in range(4):
                total = st.recv3[c, j].astype(F32) + st.partial[c, zh, j].astype(F32)
                st.recv3[c, j] = total.astype(BF16)
            return carry

        lax.fori_loop(0, 4, body, 0)
        launch(st)

    def step1(st, s):
        if s == 0:
            wire.arrived(st.recv1.at[:, 0], st.sem1[0])
        else:
            wire.arrived(st.recv1.at[:, pl.ds(1, 2)], st.sem1[1])
        for way in range(2):
            i, sign, ahead, behind = ring(st.first, way)
            c = mod4(i - sign) if s == 0 else i
            for j in range(4):
                total = st.recv1[way, s, j].astype(F32) + st.own(way, c, j).astype(F32)
                if s == 1:
                    total += st.recv1[way, 2, j].astype(F32)
                st.recv1[way, 2 * s, j] = total.astype(BF16)
            if s == 0:
                wire.put(st.recv1.at[way, 0], st.recv1.at[way, 2], behind, st.send1, st.sem1[1])
        if s == 1:
            for way in range(2):
                i, sign, ahead, behind = ring(st.second, way)
                src = st.recv1.at[way, 2, mod4(i + 2)]
                wire.put(src, st.recv2.at[way, 0], behind, st.send2, st.sem2[0])
            for way in range(2):
                i, sign, ahead, behind = ring(st.second, way)
                src = st.recv1.at[way, 2, mod4(i + sign)]
                wire.put(src, st.recv2.at[way, 1], ahead, st.send2, st.sem2[1])

    def step2(st, s):
        if s == 0:
            wire.arrived(st.recv2.at[:, 0], st.sem2[0])
        else:
            wire.arrived(st.recv2.at[:, pl.ds(1, 2)], st.sem2[1])
        for way in range(2):
            i, sign, ahead, behind = ring(st.second, way)
            c = mod4(i - sign) if s == 0 else i
            total = st.recv2[way, s].astype(F32) + st.recv1[way, 2, c].astype(F32)
            if s == 0:
                st.recv2[way, 0] = total.astype(BF16)
                wire.put(st.recv2.at[way, 0], st.recv2.at[way, 2], behind, st.send2, st.sem2[1])
                continue
            total += st.recv2[way, 2].astype(F32)
            if st.far:
                rows, cols = total.shape
                if st.recv3.shape[-2] == rows:
                    st.sums.put(slice(None), st.c0 + cols * way, total)
                else:
                    st.sums.put(slice(rows * way, rows * way + rows), st.c0, total)
            else:
                st.recv2[way, 2] = total.astype(BF16)
        if s == 1 and not st.far:
            wire.put(st.recv2.at[1 - zh, 2], st.recv3, z_far, st.send3, st.sem3)

    def result(st):
        wire.arrived(st.recv3, st.sem3)
        total = st.recv2[zh, 2].astype(F32) + st.recv3[...].astype(F32)
        st.sums.put(slice(None), st.c0, total)

    rc_send, rc_far, rc_near = wire.group(rc), wire.sem(), wire.sem()
    rz_send, rz_in = wire.group(rz), wire.sem()
    cg_send, cg_sem = wire.group(cg_rows.at[pl.ds(1, 3)]), wire.sem()

    def row_part(half, q):
        r0 = 256 * half

        def body(n, carry):
            cols = pl.ds(pl.multiple_of(q * 512 + n * 256, 256), 256)
            r = nt(gd[r0 : r0 + 256, :], wg[cols, :]) + nt(ud[r0 : r0 + 256, :], wu[cols, :])
            rg[r0 : r0 + 256, cols] = r.astype(BF16)
            return carry

        lax.fori_loop(0, 2, body, 0, unroll=True)
        if q == 3:
            if half == 1:
                wire.put(slot_rows(rg, 3), rc.at[1], mate, rc_send, rc_far)
            else:
                wire.put(slot_rows(rg, 1), rc.at[0], mate, rc_send, rc_near)

    def add_far():
        wire.arrived(rc.at[1], rc_far)

        def body(i, carry):
            rows = pl.ds(pl.multiple_of(i * 16, 16), 16)
            full = pl.ds(pl.multiple_of(2 * T + i * 16, 16), 16)
            total = rg[full, :].astype(F32) + rc[1, rows, :].astype(F32)
            rg[full, :] = total.astype(BF16)
            return carry

        lax.fori_loop(0, T // 16, body, 0)
        wire.put(slot_rows(rg, 2), rz, z_near, rz_send, rz_in)

    def add_rows():
        wire.arrived(rc.at[0], rc_near)
        wire.arrived(rz, rz_in)

        def body(i, carry):
            rows = pl.ds(pl.multiple_of(i * 16, 16), 16)
            total = rg[rows, :].astype(F32) + rc[0, rows, :].astype(F32)
            ig_out[rows, :] = (total + rz[rows, :].astype(F32)).astype(BF16)
            return carry

        lax.fori_loop(0, T // 16, body, 0)

    def combine_part():
        for slot in range(4):
            part = jnp.transpose(cg_part[slot * T : slot * T + T, :])
            cg_rows[slot] = jnp.broadcast_to(jnp.sum(part, axis=0, keepdims=True), (8, T))
        for j, to in ((1, mate), (2, z_near), (3, z_diag)):
            wire.put(cg_rows.at[j], cg_in.at[j], to, cg_send, cg_sem)

    def combine_result():
        wire.arrived(cg_in.at[pl.ds(1, 3)], cg_sem)
        answer = jnp.zeros((2, T), F32)
        for j in range(4):
            row = cg_rows[0, 0:1, :] if j == 0 else cg_in[j, 0:1, :]
            answer += jnp.where(ids_ref[...] == jnp.bitwise_xor(ex, j), row, 0.0)
        cg_out[...] = answer

    other_matmul(1)
    pass_dy(1)
    other_pointwise(1)
    down_part(0)
    pass_dy(2)
    turned(256)
    pass_dy(3)
    down_part(1)
    down_part(2)
    pass_dy(4)
    down_part(3)
    pass_dy(5)
    hidden_part(256, True, 0, 512)
    step1(d[0], 0)
    hidden_part(256, False, 512, 512)
    pass_dy(6)
    down_part(4)
    step1(d[1], 0)
    down_part(5)
    pass_dy(7)
    hidden_part(256, False, 1024, 512)
    step1(d[2], 0)
    down_part(6)
    step1(d[3], 0)
    down_part(7)
    step1(d[0], 1)
    hidden_part(256, False, 1536, 512)
    backward(256)
    step1(d[4], 0)
    up_first(up[0])
    far_first(0)
    step1(d[5], 0)
    far_first(1)
    up_first(up[1])
    up_first(up[2])
    up_first(up[3])
    step1(d[1], 1)
    step1(d[2], 1)
    far_part(0, zh)
    far_part(1, zh)
    launch_relay(narrow)
    step2(d[0], 0)
    launch_direct(narrow)
    up_rest(up[1])
    step1(d[4], 1)
    up_rest(up[3])
    step1(d[6], 0)
    up_rest(up[2])
    far_sum(far_down)
    step1(d[3], 1)
    combine_part()
    row_part(1, 0)
    step1(up[1], 0)
    row_part(1, 1)
    row_part(1, 2)
    step1(up[2], 0)
    step2(d[1], 0)
    step1(up[3], 0)
    step1(d[6], 1)
    far_sum(far[0])
    up_rest(up[0])
    step1(up[0], 0)
    step1(narrow, 0)
    step2(d[0], 1)
    step1(d[5], 1)
    step2(d[2], 0)
    step1(far_down, 0)
    row_part(1, 3)
    step2(d[4], 0)
    row_part(0, 0)
    row_part(0, 1)
    far_sum(far[1])
    step1(up[2], 1)
    row_part(0, 2)
    step2(d[1], 1)
    row_part(0, 3)
    add_far()
    step1(far[0], 0)
    step2(d[3], 0)
    far_sum(far[2])
    step1(up[3], 1)
    step1(up[0], 1)
    step2(d[5], 0)
    step2(d[6], 0)
    step1(far_down, 1)
    step1(up[1], 1)
    result(d[1])
    step1(narrow, 1)
    step1(far[0], 1)
    step2(d[2], 1)
    step2(d[3], 1)
    step1(far[2], 0)
    step1(far[1], 0)
    step2(up[3], 0)
    step2(up[2], 0)
    step2(d[5], 1)
    step2(up[0], 0)
    step2(up[1], 0)
    step2(d[4], 1)
    step2(d[6], 1)
    step2(narrow, 0)
    step2(far[0], 0)
    step1(far[2], 1)
    step1(far[1], 1)
    step2(up[3], 1)
    step2(up[2], 1)
    step2(far_down, 0)
    step2(up[0], 1)
    add_rows()
    step2(up[1], 1)
    result(d[2])
    combine_result()
    result(d[3])
    result(d[5])
    step2(narrow, 1)
    step2(far[0], 1)
    result(d[4])
    result(d[6])
    step2(far[2], 0)
    step2(far[1], 0)
    result(d[0])
    result(up[3])
    step2(far_down, 1)
    result(up[0])
    step2(far[2], 1)
    step2(far[1], 1)
    result(up[1])
    result(up[2])
    result(narrow)

    wire.finish()


def hand_over(*refs):
    for src, dst in zip(refs[:5], refs[5:]):
        dst[...] = src[...]


OUTS = (
    jax.ShapeDtypeStruct((T, D), BF16),
    jax.ShapeDtypeStruct((2, T), F32),
    jax.ShapeDtypeStruct((1, 64, FF), BF16),
    jax.ShapeDtypeStruct((1, 64, FF), BF16),
    jax.ShapeDtypeStruct((1, 24, D), BF16),
)


def shards(tokens, cotangent, expert_ids, combine, w_gate, w_up, w_down):
    hbm = pl.BlockSpec(memory_space=pl.ANY)
    vmem = pl.BlockSpec(memory_space=pltpu.VMEM)
    outs = pl.pallas_call(
        kernel,
        out_shape=tuple(pltpu.VMEM(o.shape, o.dtype) for o in OUTS),
        in_specs=[hbm] * 7,
        out_specs=(vmem,) * 5,
        scratch_shapes=[
            pltpu.VMEM((D, FF), BF16),
            pltpu.VMEM((D, FF), BF16),
            pltpu.VMEM((FF, D), BF16),
            pltpu.VMEM((4 * T, D), BF16),
            pltpu.VMEM((4 * T, D), BF16),
            pltpu.VMEM((D, 4 * T), BF16),
            pltpu.VMEM((256, FF), F32),
            pltpu.VMEM((256, FF), F32),
            pltpu.VMEM((256, FF), F32),
            pltpu.VMEM((256, FF), F32),
            pltpu.VMEM((256, FF), BF16),
            pltpu.VMEM((FF, 4 * T), BF16),
            pltpu.VMEM((4 * T, FF), BF16),
            pltpu.VMEM((4 * T, FF), BF16),
            pltpu.VMEM((4, 8, T), F32),
            pltpu.VMEM((4 * T, T), F32),
            pltpu.VMEM((4 * T, T), F32),
            pltpu.VMEM((4, 8, T), F32),
            pltpu.VMEM((4, 8, T), F32),
            pltpu.VMEM((4 * T, D), BF16),
            pltpu.VMEM((2, T, D), BF16),
            pltpu.VMEM((T, D), BF16),
            pltpu.VMEM((8, 4, 2, 4, 24, 256), BF16),
            pltpu.VMEM((4, 4, 2, 4, 64, 256), BF16),
            pltpu.VMEM((4, 4, 2, 4, 64, 128), BF16),
            pltpu.VMEM((7, 2, 3, 4, 24, 256), BF16),
            pltpu.VMEM((4, 2, 3, 4, 64, 256), BF16),
            pltpu.VMEM((3, 2, 3, 4, 32, 128), BF16),
            pltpu.VMEM((7, 2, 3, 24, 256), BF16),
            pltpu.VMEM((4, 2, 3, 64, 256), BF16),
            pltpu.VMEM((3, 2, 3, 32, 128), BF16),
            pltpu.VMEM((7, 24, 256), BF16),
            pltpu.VMEM((4, 64, 256), BF16),
            pltpu.VMEM((3, 4, 4, 64, 128), BF16),
            pltpu.VMEM((2, 3, 4, 24, 128), BF16),
            pltpu.VMEM((2, 3, 24, 128), BF16),
            pltpu.VMEM((4, 4, 24, 256), BF16),
            pltpu.VMEM((2, 3, 4, 64, 128), BF16),
            pltpu.VMEM((2, 3, 64, 128), BF16),
            pltpu.VMEM((64, 128), BF16),
            pltpu.VMEM((2, T), jnp.int32),
            pltpu.VMEM((2, T), F32),
            pltpu.SemaphoreType.DMA((7,)),
            pltpu.SemaphoreType.DMA((N_SEM,)),
        ],
        compiler_params=pltpu.CompilerParams(
            collective_id=0, has_side_effects=True, vmem_limit_bytes=60 * 1024 * 1024
        ),
        name="experts",
    )(tokens, cotangent, expert_ids.T, combine.T, w_gate, w_up, w_down)
    outs = pl.pallas_call(
        hand_over,
        out_shape=OUTS,
        in_specs=[vmem] * 5,
        out_specs=(vmem,) * 5,
        name="hand_over",
    )(*(pltpu.with_memory_space_constraint(o, pltpu.VMEM) for o in outs))
    return (outs[0], outs[1].T, *outs[2:])


def solution(mesh):
    both = ("dp", "expert")
    return jax.shard_map(
        shards,
        mesh=mesh,
        in_specs=(
            P(both, None),
            P(both, None),
            P(both, None),
            P(both, None),
            P("expert", None, None),
            P("expert", None, None),
            P("expert", None, None),
        ),
        out_specs=(
            P(both, None),
            P(both, None),
            P("expert", "dp", None),
            P("expert", "dp", None),
            P("expert", "dp", None),
        ),
        check_vma=False,
    )
```
